256 devices in a mesh: seq: 64 (over z, y, core), head: 4 (over x).
Axes of the slice: x: 4, y: 4, z: 8, core: 2. Of those that a mesh axis runs over, the one named last changes fastest.
Arguments:
- residual: bfloat16 [32768, 3072], P('seq', 'head'), may hold values from -6 to 6
- q_self: bfloat16 [32768, 3072], P('seq', 'head'), may hold values from -6 to 6
- k_self: bfloat16 [32768, 3072], P('seq', 'head'), may hold values from -6 to 6
- v_self: bfloat16 [32768, 3072], P('seq', 'head'), may hold values from -6 to 6
- w_out: bfloat16 [3072, 3072], P('head'), may hold values from -0.109375 to 0.109375
- norm_gain: float32 [3072], replicated, may hold values from 0.5 to 1.5
- w_query: bfloat16 [3072, 3072], P('seq', 'head')
- w_cache: bfloat16 [3072, 2048], P('seq', 'head')
- block_doc: int32 [64], replicated, may hold values from 0 to 15, never falling along the last dimension, each value on 1 to 5 neighbouring positions
- tail_len: int32 [64], replicated, may hold values from 1 to 512
Outputs:
- hidden: bfloat16 [32768, 3072], P('seq', 'head')
- cross_context: bfloat16 [32768, 3072], P('seq', 'head')
The draws below stay inside these ranges and needn't reach their ends.
Inputs may be any that keep to these rules, and one draw needn't show every extreme that they name: block_doc never falls along the blocks; each document covers 1 to 5 consecutive blocks, and some document covers exactly 5. `tail_len`: read only for the last block of a document.
All inputs are finite; a program needn't handle non-finite values.
Results may differ from the reference program's by a relative error of at most 0.0078.
Values may be sent and summed in bfloat16 or wider, within the bound.
A program may use at most 128 MiB of HBM per device.

```python
import math
import jax
import jax.numpy as jnp
import numpy as np
from jax import lax

D = 3072
HEADS = 24
KV_HEADS = 8
HEAD_DIM = 128
TOK_DEV = 512
WINDOW = 2048
DOC_MAX = 2560
WIN_BLOCKS = 4
DOC_BLOCKS = 5
NBLK = 64
TOKENS = 32768
SPAN_MAX = 5
DOC_COUNT = 16
N_HEAD = 4


def sign_vector(key, length):
    return jnp.where(jax.random.randint(key, (length,), 0, 2) == 0, -1.0, 1.0).astype(jnp.float32)


def picked_rows(key):
    every = max(2, TOK_DEV // 64)
    return jax.random.randint(key, (TOKENS,), 0, TOK_DEV) < every


def base_noise(key, shape):
    return jax.random.normal(jax.random.fold_in(key, 3), shape, jnp.float32)


def self_operand(key, member):
    width = HEADS * HEAD_DIM
    plan = jax.random.fold_in(key, 9001)
    picked = picked_rows(jax.random.fold_in(plan, 1))
    pattern = sign_vector(jax.random.fold_in(plan, 2), width)
    strength = jax.random.uniform(jax.random.fold_in(plan, 3), (TOKENS,), jnp.float32, 3.0, 5.5)
    spread = 0.4
    noise = base_noise(jax.random.fold_in(key, member), (TOKENS, width))
    aligned = strength[:, None] * pattern[None, :] + spread * noise
    mixed = jnp.where(picked[:, None], aligned, noise)
    return jnp.clip(mixed, -6.0, 6.0).astype(jnp.bfloat16)


def draw_q_self(key, part):
    return self_operand(key, 11)


def draw_k_self(key, part):
    return self_operand(key, 12)


def cross_patterns(key):
    plan = jax.random.fold_in(key, 9002)
    return (sign_vector(jax.random.fold_in(plan, 1), D), sign_vector(jax.random.fold_in(plan, 2), HEAD_DIM))


def draw_residual(key, part):
    feature_sign = cross_patterns(key)[0]
    plan = jax.random.fold_in(key, 9003)
    picked = picked_rows(jax.random.fold_in(plan, 1))
    strength = jax.random.uniform(jax.random.fold_in(plan, 2), (TOKENS,), jnp.float32, 2.0, 4.5)
    noise = base_noise(jax.random.fold_in(key, 13), (TOKENS, D))
    aligned = strength[:, None] * feature_sign[None, :] + 0.3 * noise
    mixed = jnp.where(picked[:, None], aligned, noise)
    return jnp.clip(mixed, -6.0, 6.0).astype(jnp.bfloat16)


def scaled_noise(key, columns):
    limit = 6.0 * D ** (-0.5)
    return jnp.clip(base_noise(key, (D, columns)) * D ** (-0.5), -limit, limit)


def draw_w_query(key, part):
    feature_sign, head_sign = cross_patterns(key)
    width = HEADS * HEAD_DIM
    noise = scaled_noise(jax.random.fold_in(key, 14), width)
    amounts = jax.random.uniform(jax.random.fold_in(key, 9005), (HEADS,), jnp.float32, 14.5, 24.5)
    columns = (amounts[:, None] * head_sign[None, :]).reshape(width)
    plant = feature_sign[:, None] * columns[None, :] / (D * HEAD_DIM ** 0.25)
    return (noise + plant).astype(jnp.bfloat16)


def draw_w_cache(key, part):
    feature_sign, head_sign = cross_patterns(key)
    group = KV_HEADS // N_HEAD
    width = 2 * KV_HEADS * HEAD_DIM
    noise = scaled_noise(jax.random.fold_in(key, 15), width)
    key_part = jnp.broadcast_to(16.0 * head_sign, (N_HEAD, group, HEAD_DIM))
    columns = jnp.stack([key_part, jnp.zeros_like(key_part)], axis=1).reshape(width)
    plant = feature_sign[:, None] * columns[None, :] / (D * HEAD_DIM ** 0.25)
    return (noise + plant).astype(jnp.bfloat16)


def with_ends(drawn, own_key, least, top_value):
    place = [jax.random.randint(jax.random.fold_in(own_key, axis), (), 0, length) for axis, length in enumerate(drawn.shape)]
    longest = drawn.shape.index(max(drawn.shape))
    next_to = place[:longest] + [(place[longest] + 1) % drawn.shape[longest]] + place[longest + 1:]
    return drawn.at[tuple(place)].set(least).at[tuple(next_to)].set(top_value)


def block_levels(own_key, shape, cuts, least, largest):
    factor_of = 1.0
    for axis_at, blocks in cuts:
        steps = jax.random.uniform(jax.random.fold_in(jax.random.fold_in(own_key, 6), axis_at), (blocks,), jnp.float32, least / len(cuts), largest / len(cuts))
        factor_of = factor_of * jnp.repeat(jnp.exp(steps), shape[axis_at] // blocks).reshape((-1,) + (1,) * (len(shape) - 1 - axis_at))
    return factor_of


def profile(count, total, most, lean):
    loads = [(1 << 20) // math.isqrt(standing ** lean) + 1 for standing in range(2, count + 1)]
    rest, holding = total - most - (count - 1), [1] * (count - 1)
    while rest > 0:
        free = [i for i in range(count - 1) if holding[i] < most]
        mass, remaining = sum([loads[i] for i in free]), rest
        for i in free:
            addition = min(most - holding[i], max(1, remaining * loads[i] // mass), rest)
            holding[i] = holding[i] + addition
            rest = rest - addition
    return np.array([most] + holding)


def uneven(own_key, amount, total, reach, lean):
    if amount == 2:
        one = jax.random.randint(own_key, (), max(1, total - reach), min(reach, total - 1) + 1)
        return jnp.stack([one, total - one])
    sizes = jnp.asarray(profile(amount, total, reach, lean), jnp.int32)
    pairs = (amount - 1) // 2
    giver, receiver = sizes[1:1 + 2 * pairs:2], sizes[2:2 + 2 * pairs:2]
    slack = jnp.minimum(giver - 1, reach - receiver)
    shifted = jax.random.randint(jax.random.fold_in(own_key, 1), (pairs,), 0, 1 << 20) % (slack + 1)
    sizes = sizes.at[1:1 + 2 * pairs:2].set(giver - shifted).at[2:2 + 2 * pairs:2].set(receiver + shifted)
    return sizes[jax.random.permutation(jax.random.fold_in(own_key, 2), amount)]


def bell_draw(stream_key, extent, scale, most, cuts=(), kind=jnp.bfloat16):
    entries = scale * jax.random.normal(stream_key, extent, jnp.float32)
    if cuts:
        entries = entries * block_levels(stream_key, extent, cuts, -0.22, 0.18)
    return jnp.clip(entries, -most, most).astype(kind)


def setup_inputs(seed: int = 0) -> dict:
    arg_keys = jax.random.split(jax.random.key(seed), 11)
    residual = draw_residual(jax.random.fold_in(arg_keys[10], 71), 0)
    q_self = draw_q_self(jax.random.fold_in(arg_keys[10], 71), 0)
    k_self = draw_k_self(jax.random.fold_in(arg_keys[10], 71), 0)
    v_self = bell_draw(arg_keys[3], (TOKENS, HEADS * HEAD_DIM), 1.0, 6.0, ((0, 64), (1, 4)))
    w_out = bell_draw(arg_keys[4], (HEADS * HEAD_DIM, D), (HEADS * HEAD_DIM) ** -0.5, 0.109375, ((0, 4),))
    norm_gain = jnp.clip(1.0 + 0.1 * jax.random.normal(arg_keys[5], (D,), jnp.float32), 0.5, 1.5)
    w_query = draw_w_query(jax.random.fold_in(arg_keys[10], 71), 0)
    w_cache = draw_w_cache(jax.random.fold_in(arg_keys[10], 71), 0)
    block_doc = jnp.searchsorted(jnp.cumsum(uneven(arg_keys[8], DOC_COUNT, NBLK, SPAN_MAX, 2)), jnp.arange(NBLK), side="right").astype(jnp.int32)
    tail_len = with_ends(jax.random.randint(arg_keys[9], (NBLK,), 1, TOK_DEV + 1), jax.random.fold_in(arg_keys[9], 1), 1, TOK_DEV).astype(jnp.int32)
    return dict(residual=residual, q_self=q_self, k_self=k_self, v_self=v_self, w_out=w_out, norm_gain=norm_gain, w_query=w_query, w_cache=w_cache, block_doc=block_doc, tail_len=tail_len)


EPSILON = 1e-06

def block_valid(block_doc, tail_len, tok_rows):
    following = jnp.concatenate([block_doc[1:], jnp.full((1,), -1, jnp.int32)])
    closing = following != block_doc
    within = jnp.arange(tok_rows, dtype=jnp.int32)
    return jnp.logical_or(jnp.logical_not(closing)[:, None], within[None, :] < tail_len[:, None])

def permitted(query_block, key_blocks, block_doc, valid_tokens, tok_rows, reach_tokens):
    inside = key_blocks >= 0
    safe_blocks = jnp.maximum(key_blocks, 0)
    own_doc = jnp.take(block_doc, query_block)
    same_doc = jnp.logical_and(inside, jnp.take(block_doc, safe_blocks) == own_doc)
    live_keys = jnp.logical_and(same_doc[:, None], jnp.take(valid_tokens, safe_blocks, axis=0))
    within = jnp.arange(tok_rows, dtype=jnp.int32)
    query_pos = query_block * tok_rows + within
    key_pos = (key_blocks[:, None] * tok_rows + within[None, :]).reshape(-1)
    distance = query_pos[:, None] - key_pos[None, :]
    near = jnp.logical_and(distance >= 0, distance < reach_tokens)
    return jnp.logical_and(near, live_keys.reshape(-1)[None, :])

def attend(queries, keys, values, allowed):
    row_count, head_count, head_dim = queries.shape
    group_size = head_count // keys.shape[1]
    scaling = 1.0 / math.sqrt(head_dim)

    def one_head(head_index):
        query_head = lax.dynamic_index_in_dim(queries, head_index, 1, keepdims=False)
        key_head = lax.dynamic_index_in_dim(keys, head_index // group_size, 1, keepdims=False)
        value_head = lax.dynamic_index_in_dim(values, head_index // group_size, 1, keepdims=False)
        scores = lax.dot_general(query_head, key_head, (((1,), (1,)), ((), ())), preferred_element_type=jnp.float32) * scaling
        scores = jnp.where(allowed, scores, -1e+30)
        row_peak = lax.optimization_barrier(jnp.max(scores, axis=1, keepdims=True))
        weights = jnp.exp(scores - row_peak)
        row_total = lax.optimization_barrier(jnp.sum(weights, axis=1, keepdims=True))
        blended = jnp.dot(weights.astype(jnp.bfloat16), value_head, preferred_element_type=jnp.float32)
        return (blended / row_total).astype(jnp.bfloat16)
    per_head = lax.map(one_head, jnp.arange(head_count, dtype=jnp.int32))
    return jnp.transpose(per_head, (1, 0, 2)).reshape(row_count, head_count * head_dim)

def reference(residual, q_self, k_self, v_self, w_out, norm_gain, w_query, w_cache, block_doc, tail_len):
    valid_tokens = block_valid(block_doc, tail_len, TOK_DEV)
    width_all = HEADS * HEAD_DIM
    win_rows = WIN_BLOCKS * TOK_DEV
    key_pad = jnp.concatenate([jnp.zeros((win_rows, width_all), jnp.bfloat16), k_self], axis=0)
    value_pad = jnp.concatenate([jnp.zeros((win_rows, width_all), jnp.bfloat16), v_self], axis=0)

    def self_block(block_index):
        row_start = block_index * TOK_DEV
        queries = lax.dynamic_slice_in_dim(q_self, row_start, TOK_DEV, 0).reshape(TOK_DEV, HEADS, HEAD_DIM)
        keys = lax.dynamic_slice_in_dim(key_pad, row_start, win_rows + TOK_DEV, 0).reshape(-1, HEADS, HEAD_DIM)
        values = lax.dynamic_slice_in_dim(value_pad, row_start, win_rows + TOK_DEV, 0).reshape(-1, HEADS, HEAD_DIM)
        key_blocks = block_index - WIN_BLOCKS + jnp.arange(WIN_BLOCKS + 1, dtype=jnp.int32)
        allowed = permitted(block_index, key_blocks, block_doc, valid_tokens, TOK_DEV, WINDOW)
        return attend(queries, keys, values, allowed)
    context = lax.map(self_block, jnp.arange(NBLK, dtype=jnp.int32)).reshape(TOKENS, width_all)
    projected = jnp.dot(context, w_out, preferred_element_type=jnp.float32)
    hidden = (residual.astype(jnp.float32) + projected).astype(jnp.bfloat16)
    wide = hidden.astype(jnp.float32)
    mean_square = lax.optimization_barrier(jnp.mean(wide * wide, axis=1, keepdims=True))
    normed = (wide * lax.rsqrt(mean_square + EPSILON) * norm_gain).astype(jnp.bfloat16)
    cross_queries = jnp.dot(normed, w_query, preferred_element_type=jnp.float32).astype(jnp.bfloat16)
    cache_rows = jnp.dot(normed, w_cache, preferred_element_type=jnp.float32).astype(jnp.bfloat16)
    cache_rows = cache_rows.reshape(TOKENS, N_HEAD, 2, KV_HEADS // N_HEAD, HEAD_DIM)
    cache_keys = cache_rows[:, :, 0].reshape(TOKENS, KV_HEADS * HEAD_DIM)
    cache_values = cache_rows[:, :, 1].reshape(TOKENS, KV_HEADS * HEAD_DIM)
    doc_rows = (DOC_BLOCKS - 1) * TOK_DEV
    cache_key_pad = jnp.concatenate([jnp.zeros((doc_rows, KV_HEADS * HEAD_DIM), jnp.bfloat16), cache_keys], axis=0)
    cache_value_pad = jnp.concatenate([jnp.zeros((doc_rows, KV_HEADS * HEAD_DIM), jnp.bfloat16), cache_values], axis=0)

    def cross_block(block_index):
        row_start = block_index * TOK_DEV
        queries = lax.dynamic_slice_in_dim(cross_queries, row_start, TOK_DEV, 0).reshape(TOK_DEV, HEADS, HEAD_DIM)
        keys = lax.dynamic_slice_in_dim(cache_key_pad, row_start, doc_rows + TOK_DEV, 0).reshape(-1, KV_HEADS, HEAD_DIM)
        values = lax.dynamic_slice_in_dim(cache_value_pad, row_start, doc_rows + TOK_DEV, 0).reshape(-1, KV_HEADS, HEAD_DIM)
        key_blocks = block_index - DOC_BLOCKS + 1 + jnp.arange(DOC_BLOCKS, dtype=jnp.int32)
        allowed = permitted(block_index, key_blocks, block_doc, valid_tokens, TOK_DEV, DOC_MAX)
        return attend(queries, keys, values, allowed)
    cross_context = lax.map(cross_block, jnp.arange(NBLK, dtype=jnp.int32)).reshape(TOKENS, width_all)
    return (hidden, cross_context)
```

```python
import functools
import math

import jax
import jax.numpy as jnp
from jax import lax
from jax.experimental import pallas as pl
from jax.experimental.pallas import tpu as pltpu
from jax.sharding import PartitionSpec as P

D = 3072
HEAD_DIM = 128
ROWS = 512
NBLK = 64
HEADS = 6
SLOTS = 5
WIDTH = HEADS * HEAD_DIM
HALF = WIDTH // 2
EPSILON = 1e-06
SCALE = 1.0 / math.sqrt(HEAD_DIM)
MASKED = -1e30
TILE = 128

MESH = pl.DeviceIdType.MESH
F32 = jnp.float32
BF16 = jnp.bfloat16

PLUS = (0, 3)
MINUS = (1, 2, 4, 5)


class Copies:
    def __init__(self, send_sem, recv_sem):
        self.send_sem, self.recv_sem = send_sem, recv_sem
        self.made = {}

    def make(self, name, src, dst, device):
        if name not in self.made:
            self.made[name] = len(self.made)
        n = self.made[name]
        return pltpu.make_async_remote_copy(
            src_ref=src,
            dst_ref=dst,
            send_sem=self.send_sem.at[n],
            recv_sem=self.recv_sem.at[n],
            device_id=device,
            device_id_type=MESH,
        )


class Place:
    def __init__(self):
        i = lax.axis_index("seq")
        x = lax.axis_index("head")
        self.i, self.x = i, x
        c = i % 2
        y = (i // 2) % 4
        z = i // 8
        self.c, self.y, self.z = c, y, z

        def at(zz, yy, cc):
            return ((zz + 8) % 8 * 4 + yy) * 2 + cc

        up = (y + 1) % 4
        down = (y + 3) % 4
        self.next_chip = (at(z + (y + 1) // 4, up, c), x)
        self.prev_chip = (at(z - (6 - y) // 6, down, c), x)
        self.relay_to = (at(z, down, c), x)
        self.relay_from = (at(z, up, c), x)
        self.pass_to = (at(z + (up + 2) // 4, down, c), x)
        self.pass_from = (at(z - ((y + 2) % 4) // 2, up, c), x)
        self.partner = (i + 1 - 2 * c, x)
        self.right = (i, (x + 1) % 4)
        self.left = (i, (x + 3) % 4)


def greet(devices):
    barrier = pltpu.get_barrier_semaphore()
    for device in devices:
        pl.semaphore_signal(barrier, inc=1, device_id=device, device_id_type=MESH)
    pl.semaphore_wait(barrier, len(devices))


def key_limits(doc_ref, tail_ref, i):
    limits = []
    own = doc_ref[i]
    for d in range(SLOTS):
        j = jnp.maximum(i - d, 0)
        doc = doc_ref[j]
        after = doc_ref[jnp.minimum(j + 1, NBLK - 1)]
        closing = jnp.logical_or(j == NBLK - 1, after != doc)
        count = jnp.where(closing, tail_ref[j], ROWS)
        seen = jnp.logical_and(i - d >= 0, doc == own)
        limits.append(jnp.where(seen, count, 0))
    return limits


def attend_tile(q, keys, values, limits, row0, windowed):
    rows = q.shape[0]
    query_at = row0 + lax.broadcasted_iota(jnp.int32, (rows, ROWS), 0)
    key_at = lax.broadcasted_iota(jnp.int32, (rows, ROWS), 1)
    lane = lax.broadcasted_iota(jnp.int32, (1, ROWS), 1)
    scores = []
    for d in range(SLOTS):
        s = lax.dot_general(q, keys(d), (((1,), (1,)), ((), ())), preferred_element_type=F32)
        s = s * SCALE + jnp.where(lane < limits[d], 0.0, MASKED)
        if d == 0:
            s = jnp.where(key_at <= query_at, s, MASKED)
        if d == SLOTS - 1 and windowed:
            s = jnp.where(key_at > query_at, s, MASKED)
        scores.append(s)
    peak = functools.reduce(jnp.maximum, scores)
    peak = jnp.max(peak, axis=1, keepdims=True)
    total = None
    blended = None
    for d in range(SLOTS):
        weights = jnp.exp(scores[d] - peak)
        total = weights if total is None else total + weights
        part = jnp.dot(weights.astype(BF16), values(d), preferred_element_type=F32)
        blended = part if blended is None else blended + part
    return (blended / jnp.sum(total, axis=1, keepdims=True)).astype(BF16)


def self_kernel(
    doc_ref, tail_ref, q_ref, res_ref, k_hbm, v_hbm, wo_hbm, hidden_ref,
    kv, relay, ctx, woc, wrelay, acc, local_sem, send_sem, recv_sem,
):
    here = Place()
    i, x, c = here.i, here.x, here.c
    copies = Copies(send_sem, recv_sem)
    started = []
    right_x, left_x, far_x = (x + 1) % 4, (x + 3) % 4, (x + 2) % 4

    local = []
    for h in range(HEADS):
        cols = pl.ds(h * HEAD_DIM, HEAD_DIM)
        one = pltpu.make_async_copy(k_hbm.at[:, cols], kv.at[SLOTS - 1, h, 0], local_sem.at[2 * h])
        two = pltpu.make_async_copy(v_hbm.at[:, cols], kv.at[SLOTS - 1, h, 1], local_sem.at[2 * h + 1])
        one.start()
        two.start()
        local.append((one, two))
    own_rows = pl.ds(pl.multiple_of(x * WIDTH, WIDTH), WIDTH)
    own_cols = pl.ds(pl.multiple_of(x * WIDTH, WIDTH), WIDTH)
    own_w = pltpu.make_async_copy(wo_hbm.at[:, own_cols], woc.at[own_rows], local_sem.at[2 * HEADS])
    own_w.start()

    greet([
        here.next_chip, here.prev_chip, here.relay_to, here.relay_from, here.pass_to, here.pass_from,
        here.partner, here.right, here.left,
    ])

    def go(copy):
        copy.start()
        started.append(copy)

    def forth(h):
        return copies.make(("forth", h), kv.at[4, h], kv.at[1, h], here.next_chip)

    def again(h):
        return copies.make(("again", h), kv.at[1, h], kv.at[3, h], here.next_chip)

    def back(h):
        return copies.make(("back", h), kv.at[4, h], relay.at[MINUS.index(h)], here.relay_to)

    def over(h):
        return copies.make(("over", h), relay.at[MINUS.index(h)], kv.at[3, h], here.pass_to)

    def twin_near(h):
        return copies.make(("near", h), kv.at[1, h], kv.at[2 * (1 - c), h], here.partner)

    def twin_far(h):
        return copies.make(("far", h), kv.at[4 - c, h], kv.at[2 * c, h], here.partner)

    def w_rows(block, first, count):
        return pl.ds(pl.multiple_of(block * WIDTH + c * HALF + first, 64), count)

    def w_cols(block):
        return pl.ds(pl.multiple_of(block * WIDTH, WIDTH), WIDTH)

    quarter = HALF // 2
    c_half = pl.ds(pl.multiple_of(c * HALF, HALF), HALF)
    c_one = pl.ds(pl.multiple_of(c * HALF, 64), quarter)
    c_two = pl.ds(pl.multiple_of(c * HALF + quarter, 64), quarter)
    w_right = copies.make("wr", wo_hbm.at[c_half, w_cols(right_x)], woc.at[w_rows(x, 0, HALF)], here.right)
    w_left = copies.make("wl", wo_hbm.at[c_half, w_cols(left_x)], woc.at[w_rows(x, 0, HALF)], here.left)
    w_far_r = copies.make("wfr", wo_hbm.at[c_one, w_cols(far_x)], wrelay.at[0], here.right)
    w_far_l = copies.make("wfl", wo_hbm.at[c_two, w_cols(far_x)], wrelay.at[1], here.left)
    w_on_r = copies.make("wor", wrelay.at[0], woc.at[w_rows(left_x, 0, quarter)], here.right)
    w_on_l = copies.make("wol", wrelay.at[1], woc.at[w_rows(right_x, quarter, quarter)], here.left)

    def w_twin(name, block):
        rows = w_rows(block, 0, HALF)
        return copies.make(("wt", name), woc.at[rows], woc.at[rows], here.partner)

    w_twin_l = w_twin("l", left_x)
    w_twin_r = w_twin("r", right_x)
    w_twin_f = w_twin("f", far_x)

    def ctx_cols(block, h):
        return pl.ds(pl.multiple_of(block * WIDTH + h * HEAD_DIM, HEAD_DIM), HEAD_DIM)

    upper, lower = pl.ds(0, ROWS // 2), pl.ds(ROWS // 2, ROWS // 2)

    def ctx_right(h):
        return copies.make(("cr", h), ctx.at[:, ctx_cols(x, h)], ctx.at[:, ctx_cols(x, h)], here.right)

    def ctx_left(h):
        return copies.make(("cl", h), ctx.at[:, ctx_cols(x, h)], ctx.at[:, ctx_cols(x, h)], here.left)

    def ctx_on_right(h):
        part = ctx.at[upper, ctx_cols(left_x, h)]
        return copies.make(("cor", h), part, part, here.right)

    def ctx_on_left(h):
        part = ctx.at[lower, ctx_cols(right_x, h)]
        return copies.make(("col", h), part, part, here.left)

    limits = key_limits(doc_ref, tail_ref, i)

    def attend(h):
        def slot(d):
            return (d + SLOTS - 1) % SLOTS

        def tile(t, carry):
            row0 = pl.multiple_of(t * TILE, TILE)
            rows = pl.ds(row0, TILE)
            q = q_ref[rows, h * HEAD_DIM:(h + 1) * HEAD_DIM]
            out = attend_tile(
                q, lambda d: kv[slot(d), h, 0], lambda d: kv[slot(d), h, 1], limits, row0, True
            )
            ctx[rows, ctx_cols(x, h)] = out
            return carry

        lax.fori_loop(0, ROWS // TILE, tile, 0)
        go(ctx_right(h))
        go(ctx_left(h))

    def pass_context(h):
        ctx_right(h).wait_recv()
        go(ctx_on_right(h))
        ctx_left(h).wait_recv()
        go(ctx_on_left(h))

    for h in (0, 1, 2):
        for copy in local[h]:
            copy.wait()
    go(forth(0))
    go(back(1))
    go(w_right)
    go(w_left)
    go(w_far_r)
    go(w_far_l)
    go(forth(1))
    go(back(2))
    for h in (3, 4, 5):
        for copy in local[h]:
            copy.wait()
    own_w.wait()

    forth(0).wait_recv()
    go(again(0))
    go(forth(3))
    go(twin_near(0))
    back(1).wait_recv()
    go(over(1))
    go(back(4))
    forth(1).wait_recv()
    go(forth(2))
    go(twin_near(1))
    back(2).wait_recv()
    go(over(2))
    go(back(5))
    again(0).wait_recv()
    go(twin_far(0))
    over(1).wait_recv()
    go(twin_far(1))
    twin_near(0).wait_recv()
    twin_far(0).wait_recv()
    attend(0)
    w_right.wait_recv()
    go(w_twin_l)
    w_left.wait_recv()
    go(w_twin_r)
    w_far_r.wait_recv()
    go(w_on_r)
    w_far_l.wait_recv()
    go(w_on_l)
    twin_near(1).wait_recv()
    twin_far(1).wait_recv()
    attend(1)
    forth(3).wait_recv()
    go(again(3))
    go(forth(4))
    go(forth(5))
    go(twin_near(3))
    back(4).wait_recv()
    go(over(4))
    forth(2).wait_recv()
    go(twin_near(2))
    over(2).wait_recv()
    go(twin_far(2))
    w_on_r.wait_recv()
    w_on_l.wait_recv()
    go(w_twin_f)
    twin_near(2).wait_recv()
    twin_far(2).wait_recv()
    attend(2)
    pass_context(0)
    pass_context(1)
    back(5).wait_recv()
    go(over(5))
    again(3).wait_recv()
    go(twin_far(3))
    twin_near(3).wait_recv()
    twin_far(3).wait_recv()
    attend(3)
    pass_context(2)
    forth(4).wait_recv()
    go(twin_near(4))
    over(4).wait_recv()
    go(twin_far(4))
    twin_near(4).wait_recv()
    twin_far(4).wait_recv()
    attend(4)
    pass_context(3)
    forth(5).wait_recv()
    go(twin_near(5))
    over(5).wait_recv()
    go(twin_far(5))
    twin_near(5).wait_recv()
    twin_far(5).wait_recv()
    attend(5)
    pass_context(4)
    for copy in (w_twin_l, w_twin_r, w_twin_f):
        copy.wait_recv()
    for h in range(4):
        ctx_on_right(h).wait_recv()
        ctx_on_left(h).wait_recv()

    def project(first, count, seed, store):
        def tile(t, carry):
            rows = pl.ds(pl.multiple_of(t * TILE, TILE), TILE)
            total = seed(rows)
            for block in range(4):
                at = block * WIDTH + first
                total = total + jnp.dot(
                    ctx[rows, at:at + count], woc[at:at + count, :], preferred_element_type=F32
                )
            store(rows, total)
            return carry

        lax.fori_loop(0, ROWS // TILE, tile, 0)

    def keep(rows, total):
        acc[rows, :] = total

    def finish(rows, total):
        hidden_ref[rows, :] = (res_ref[rows, :].astype(F32) + total).astype(BF16)

    project(0, 4 * HEAD_DIM, lambda rows: jnp.zeros((TILE, WIDTH), F32), keep)
    pass_context(5)
    for h in (4, 5):
        ctx_on_right(h).wait_recv()
        ctx_on_left(h).wait_recv()
    project(4 * HEAD_DIM, 2 * HEAD_DIM, lambda rows: acc[rows, :], finish)
    for copy in started:
        copy.wait_send()


N_SELF = 62


def self_layer(doc, tail, q, res, k, v, wo):
    any_spec = pl.BlockSpec(memory_space=pl.ANY)
    vmem = pl.BlockSpec(memory_space=pltpu.VMEM)
    smem = pl.BlockSpec(memory_space=pltpu.SMEM)
    return pl.pallas_call(
        self_kernel,
        out_shape=jax.ShapeDtypeStruct((ROWS, WIDTH), BF16),
        in_specs=[smem, smem, vmem, vmem, any_spec, any_spec, any_spec],
        out_specs=vmem,
        scratch_shapes=[
            pltpu.VMEM((SLOTS, HEADS, 2, ROWS, HEAD_DIM), BF16),
            pltpu.VMEM((len(MINUS), 2, ROWS, HEAD_DIM), BF16),
            pltpu.VMEM((ROWS, D), BF16),
            pltpu.VMEM((D, WIDTH), BF16),
            pltpu.VMEM((2, HALF // 2, WIDTH), BF16),
            pltpu.VMEM((ROWS, WIDTH), F32),
            pltpu.SemaphoreType.DMA((2 * HEADS + 1,)),
            pltpu.SemaphoreType.DMA((N_SELF,)),
            pltpu.SemaphoreType.DMA((N_SELF,)),
        ],
        compiler_params=pltpu.CompilerParams(
            collective_id=0, has_side_effects=True, vmem_limit_bytes=56 * 1024 * 1024
        ),
        cost_estimate=pl.CostEstimate(
            flops=60_000_000_000, bytes_accessed=20_000_000, transcendentals=0
        ),
        name="self_layer",
    )(doc, tail, q, res, k, v, wo)


def cross_kernel(doc_ref, tail_ref, q_ref, hist_ref, out_ref):
    i = lax.axis_index("seq")
    limits = key_limits(doc_ref, tail_ref, i)

    def slot_rows(d):
        at = (SLOTS - 1 - d) * ROWS
        return slice(at, at + ROWS)

    for h in range(HEADS):
        g = h // 3

        def tile(t, carry):
            row0 = pl.multiple_of(t * TILE, TILE)
            rows = pl.ds(row0, TILE)
            q = q_ref[rows, h * HEAD_DIM:(h + 1) * HEAD_DIM]
            out_ref[rows, h * HEAD_DIM:(h + 1) * HEAD_DIM] = attend_tile(
                q,
                lambda d: hist_ref[slot_rows(d), g * HEAD_DIM:(g + 1) * HEAD_DIM],
                lambda d: hist_ref[slot_rows(d), (2 + g) * HEAD_DIM:(3 + g) * HEAD_DIM],
                limits, row0, False,
            )
            return carry

        lax.fori_loop(0, ROWS // TILE, tile, 0)


def cross_attend(doc, tail, q, hist):
    vmem = pl.BlockSpec(memory_space=pltpu.VMEM)
    smem = pl.BlockSpec(memory_space=pltpu.SMEM)
    return pl.pallas_call(
        cross_kernel,
        out_shape=jax.ShapeDtypeStruct((ROWS, WIDTH), BF16),
        in_specs=[smem, smem, vmem, vmem],
        out_specs=vmem,
        compiler_params=pltpu.CompilerParams(vmem_limit_bytes=48 * 1024 * 1024),
        cost_estimate=pl.CostEstimate(
            flops=12_000_000_000, bytes_accessed=5_000_000, transcendentals=0
        ),
        name="cross_attend",
    )(doc, tail, q, hist)


def passed_along(block, axis, distance):
    devices = range(lax.axis_size(axis))
    route = [(i - distance, i) for i in devices if i - distance in devices]
    return lax.ppermute(block, axis, route)


def local(
    residual, q_self, k_self, v_self, w_out, norm_gain, w_query, w_cache, block_doc, tail_len
):
    weights = lax.all_gather(
        jnp.concatenate([w_query, w_cache], axis=1), "seq", axis=0, tiled=True
    )
    hidden = self_layer(block_doc, tail_len, q_self, residual, k_self, v_self, w_out)
    everything = lax.all_gather(hidden, "head", axis=1, tiled=True)
    wide = everything.astype(F32)
    mean_square = jnp.mean(wide * wide, axis=1, keepdims=True)
    normed = (wide * lax.rsqrt(mean_square + EPSILON) * norm_gain).astype(BF16)
    cache_rows = jnp.dot(normed, weights[:, WIDTH:], preferred_element_type=F32).astype(BF16)
    cross_queries = jnp.dot(normed, weights[:, :WIDTH], preferred_element_type=F32).astype(BF16)
    earlier = [passed_along(cache_rows, "seq", offset) for offset in range(SLOTS - 1, 0, -1)]
    history = jnp.concatenate(earlier + [cache_rows], axis=0)
    return (hidden, cross_attend(block_doc, tail_len, cross_queries, history))


def solution(mesh):
    in_specs = (
        P("seq", "head"),
        P("seq", "head"),
        P("seq", "head"),
        P("seq", "head"),
        P("head", None),
        P(),
        P("seq", "head"),
        P("seq", "head"),
        P(),
        P(),
    )
    out_specs = (P("seq", "head"), P("seq", "head"))
    return jax.shard_map(local, mesh=mesh, in_specs=in_specs, out_specs=out_specs, check_vma=False)
```

```python
import functools
import math

import jax
import jax.numpy as jnp
from jax import lax
from jax.experimental import pallas as pl
from jax.experimental.pallas import tpu as pltpu
from jax.sharding import PartitionSpec as P

D = 3072
HEAD_DIM = 128
ROWS = 512
NBLK = 64
HEADS = 6
SLOTS = 5
WIDTH = HEADS * HEAD_DIM
HALF = WIDTH // 2
EPSILON = 1e-06
SCALE = 1.0 / math.sqrt(HEAD_DIM)
EXP2_SCALE = SCALE * math.log2(math.e)
MASKED = -1e30
LARGE = 3.0e38
TILE = 128
GROUPS = 8
SHARD = D // NBLK
COLS = WIDTH + 2 * 2 * HEAD_DIM

MESH = pl.DeviceIdType.MESH
F32 = jnp.float32
BF16 = jnp.bfloat16

PLUS = (0, 3)
MINUS = (1, 2, 4, 5)


class Copies:
    def __init__(self, send_sem, recv_sem):
        self.send_sem, self.recv_sem = send_sem, recv_sem
        self.made = {}

    def make(self, name, src, dst, device):
        if name not in self.made:
            self.made[name] = len(self.made)
        n = self.made[name]
        return pltpu.make_async_remote_copy(
            src_ref=src,
            dst_ref=dst,
            send_sem=self.send_sem.at[n],
            recv_sem=self.recv_sem.at[n],
            device_id=device,
            device_id_type=MESH,
        )


class Place:
    def __init__(self):
        i = lax.axis_index("seq")
        x = lax.axis_index("head")
        self.i, self.x = i, x
        c = i % 2
        y = (i // 2) % 4
        z = i // 8
        self.c, self.y, self.z = c, y, z

        def at(zz, yy, cc):
            return ((zz + 8) % 8 * 4 + yy) * 2 + cc

        up = (y + 1) % 4
        down = (y + 3) % 4
        self.next_chip = (at(z + (y + 1) // 4, up, c), x)
        self.prev_chip = (at(z - (6 - y) // 6, down, c), x)
        self.relay_to = (at(z, down, c), x)
        self.relay_from = (at(z, up, c), x)
        self.pass_to = (at(z + (up + 2) // 4, down, c), x)
        self.pass_from = (at(z - ((y + 2) % 4) // 2, up, c), x)
        self.partner = (i + 1 - 2 * c, x)
        self.right = (i, (x + 1) % 4)
        self.left = (i, (x + 3) % 4)
        self.y_up, self.y_down = (at(z, up, c), x), (at(z, down, c), x)
        self.z_up, self.z_down = (at(z + 1, y, c), x), (at(z - 1, y, c), x)


def greet(devices):
    barrier = pltpu.get_barrier_semaphore()
    for device in devices:
        pl.semaphore_signal(barrier, inc=1, device_id=device, device_id_type=MESH)
    pl.semaphore_wait(barrier, len(devices))


def key_limits(doc_ref, tail_ref, i):
    limits = []
    own = doc_ref[i]
    for d in range(SLOTS):
        j = jnp.maximum(i - d, 0)
        doc = doc_ref[j]
        after = doc_ref[jnp.minimum(j + 1, NBLK - 1)]
        closing = jnp.logical_or(j == NBLK - 1, after != doc)
        count = jnp.where(closing, tail_ref[j], ROWS)
        seen = jnp.logical_and(i - d >= 0, doc == own)
        limits.append(jnp.where(seen, count, 0))
    return limits


def flash_step(q, keys, values, limit, state, past=None):
    rows = q.shape[0]
    lane = lax.broadcasted_iota(jnp.int32, (1, ROWS), 1)
    s = lax.dot_general(q, keys, (((1,), (1,)), ((), ())), preferred_element_type=F32)
    s = jnp.minimum(s, jnp.where(lane < limit, LARGE, MASKED))
    if past is not None:
        query_at = lax.broadcasted_iota(jnp.int32, (rows, ROWS), 0)
        key_at = lax.broadcasted_iota(jnp.int32, (rows, ROWS), 1)
        s = jnp.where(key_at <= query_at if past == "own" else key_at > query_at, s, MASKED)
    peak = jnp.max(s, axis=1, keepdims=True)
    if state is not None:
        peak = jnp.maximum(peak, state[0])
    weights = jnp.exp2((s - peak) * EXP2_SCALE)
    total = jnp.sum(weights, axis=1, keepdims=True)
    blended = jnp.dot(weights.astype(BF16), values, preferred_element_type=F32)
    if state is not None:
        shrink = jnp.exp2((state[0] - peak) * EXP2_SCALE)
        total = state[1] * shrink + total
        blended = state[2] * shrink + blended
    return peak, total, blended


def put_state(refs, h, state):
    peak_ref, total_ref, blended_ref = refs
    peak_ref[h] = jnp.broadcast_to(state[0], (ROWS, HEAD_DIM))
    total_ref[h] = jnp.broadcast_to(state[1], (ROWS, HEAD_DIM))
    blended_ref[h] = state[2]


def get_state(refs, h):
    peak_ref, total_ref, blended_ref = refs
    return peak_ref[h][:, :1], total_ref[h][:, :1], blended_ref[h]


STATE = [
    pltpu.VMEM((HEADS, ROWS, HEAD_DIM), F32),
    pltpu.VMEM((HEADS, ROWS, HEAD_DIM), F32),
    pltpu.VMEM((HEADS, ROWS, HEAD_DIM), F32),
]


def self_kernel(
    doc_ref, tail_ref, q_ref, res_ref, shard_ref, k_hbm, v_hbm, wo_hbm, hidden_ref, wall,
    kv, relay, ctx, woc, wrelay, acc, peak_ref, total_ref, blended_ref, local_sem, send_sem, recv_sem,
):
    refs = (peak_ref, total_ref, blended_ref)
    here = Place()
    i, x, c = here.i, here.x, here.c
    copies = Copies(send_sem, recv_sem)
    started = []
    right_x, left_x, far_x = (x + 1) % 4, (x + 3) % 4, (x + 2) % 4

    local = []
    for h in range(HEADS):
        cols = pl.ds(h * HEAD_DIM, HEAD_DIM)
        one = pltpu.make_async_copy(k_hbm.at[:, cols], kv.at[SLOTS - 1, h, 0], local_sem.at[2 * h])
        two = pltpu.make_async_copy(v_hbm.at[:, cols], kv.at[SLOTS - 1, h, 1], local_sem.at[2 * h + 1])
        one.start()
        two.start()
        local.append((one, two))
    own_rows = pl.ds(pl.multiple_of(x * WIDTH, WIDTH), WIDTH)
    own_cols = pl.ds(pl.multiple_of(x * WIDTH, WIDTH), WIDTH)
    own_w = pltpu.make_async_copy(wo_hbm.at[:, own_cols], woc.at[own_rows], local_sem.at[2 * HEADS])
    own_w.start()
    own_shard = pltpu.make_async_copy(
        shard_ref, wall.at[here.z, here.y, c], local_sem.at[2 * HEADS + 1]
    )
    own_shard.start()

    greet([
        here.next_chip, here.prev_chip, here.relay_to, here.relay_from, here.pass_to, here.pass_from,
        here.partner, here.right, here.left, here.y_up, here.y_down, here.z_up, here.z_down,
    ])

    def go(copy):
        copy.start()
        started.append(copy)

    mine = wall.at[here.z, here.y, c]
    below = wall.at[here.z, (here.y + 3) % 4, c]
    shard_up = copies.make("su", shard_ref, mine, here.y_up)
    shard_down = copies.make("sd", shard_ref, mine, here.y_down)
    shard_on = copies.make("so", below, below, here.y_up)

    def group(steps):
        return wall.at[(here.z + GROUPS + steps) % GROUPS, :, c]

    def rise(n):
        return copies.make(("rise", n), group(-n), group(-n), here.z_up)

    def sink(n):
        return copies.make(("sink", n), group(n), group(n), here.z_down)

    def share(steps):
        return copies.make(("share", steps), group(steps), group(steps), here.partner)

    def forth(h):
        return copies.make(("forth", h), kv.at[4, h], kv.at[1, h], here.next_chip)

    def again(h):
        return copies.make(("again", h), kv.at[1, h], kv.at[3, h], here.next_chip)

    def back(h):
        return copies.make(("back", h), kv.at[4, h], relay.at[MINUS.index(h)], here.relay_to)

    def over(h):
        return copies.make(("over", h), relay.at[MINUS.index(h)], kv.at[3, h], here.pass_to)

    def twin_near(h):
        return copies.make(("near", h), kv.at[1, h], kv.at[2 * (1 - c), h], here.partner)

    def twin_far(h):
        return copies.make(("far", h), kv.at[4 - c, h], kv.at[2 * c, h], here.partner)

    def w_rows(block, first, count):
        return pl.ds(pl.multiple_of(block * WIDTH + c * HALF + first, 64), count)

    def w_cols(block):
        return pl.ds(pl.multiple_of(block * WIDTH, WIDTH), WIDTH)

    quarter = HALF // 2
    c_half = pl.ds(pl.multiple_of(c * HALF, HALF), HALF)
    c_one = pl.ds(pl.multiple_of(c * HALF, 64), quarter)
    c_two = pl.ds(pl.multiple_of(c * HALF + quarter, 64), quarter)
    w_right = copies.make("wr", wo_hbm.at[c_half, w_cols(right_x)], woc.at[w_rows(x, 0, HALF)], here.right)
    w_left = copies.make("wl", wo_hbm.at[c_half, w_cols(left_x)], woc.at[w_rows(x, 0, HALF)], here.left)
    w_far_r = copies.make("wfr", wo_hbm.at[c_one, w_cols(far_x)], wrelay.at[0], here.right)
    w_far_l = copies.make("wfl", wo_hbm.at[c_two, w_cols(far_x)], wrelay.at[1], here.left)
    w_on_r = copies.make("wor", wrelay.at[0], woc.at[w_rows(left_x, 0, quarter)], here.right)
    w_on_l = copies.make("wol", wrelay.at[1], woc.at[w_rows(right_x, quarter, quarter)], here.left)

    def w_twin(name, block):
        rows = w_rows(block, 0, HALF)
        return copies.make(("wt", name), woc.at[rows], woc.at[rows], here.partner)

    w_twin_l = w_twin("l", left_x)
    w_twin_r = w_twin("r", right_x)
    w_twin_f = w_twin("f", far_x)

    def ctx_cols(block, h):
        return pl.ds(pl.multiple_of(block * WIDTH + h * HEAD_DIM, HEAD_DIM), HEAD_DIM)

    upper, lower = pl.ds(0, ROWS // 2), pl.ds(ROWS // 2, ROWS // 2)

    def ctx_right(h):
        return copies.make(("cr", h), ctx.at[:, ctx_cols(x, h)], ctx.at[:, ctx_cols(x, h)], here.right)

    def ctx_left(h):
        return copies.make(("cl", h), ctx.at[:, ctx_cols(x, h)], ctx.at[:, ctx_cols(x, h)], here.left)

    def ctx_on_right(h):
        part = ctx.at[upper, ctx_cols(left_x, h)]
        return copies.make(("cor", h), part, part, here.right)

    def ctx_on_left(h):
        part = ctx.at[lower, ctx_cols(right_x, h)]
        return copies.make(("col", h), part, part, here.left)

    limits = key_limits(doc_ref, tail_ref, i)

    near_limit = jnp.where(c == 0, limits[1], limits[3])
    far_limit = jnp.where(c == 0, limits[3], limits[1])

    def first_keys(h):
        q = q_ref[:, h * HEAD_DIM:(h + 1) * HEAD_DIM]
        state = flash_step(q, kv[4, h, 0], kv[4, h, 1], limits[0], None, "own")
        state = flash_step(q, kv[1, h, 0], kv[1, h, 1], limits[2], state)
        near = 2 * c
        state = flash_step(q, kv[near, h, 0], kv[near, h, 1], near_limit, state)
        put_state(refs, h, state)

    def last_keys(h):
        q = q_ref[:, h * HEAD_DIM:(h + 1) * HEAD_DIM]
        state = get_state(refs, h)
        state = flash_step(q, kv[3, h, 0], kv[3, h, 1], limits[4], state, "edge")
        far = 2 * (1 - c)
        state = flash_step(q, kv[far, h, 0], kv[far, h, 1], far_limit, state)
        ctx[:, ctx_cols(x, h)] = (state[2] / state[1]).astype(BF16)
        go(ctx_right(h))
        go(ctx_left(h))

    def pass_context(h):
        ctx_right(h).wait_recv()
        go(ctx_on_right(h))
        ctx_left(h).wait_recv()
        go(ctx_on_left(h))

    go(shard_up)
    go(shard_down)
    for h in (0, 1, 2):
        for copy in local[h]:
            copy.wait()
    go(forth(0))
    go(back(1))
    go(w_right)
    go(w_left)
    go(w_far_r)
    go(w_far_l)
    go(forth(1))
    go(back(2))
    for h in (3, 4, 5):
        for copy in local[h]:
            copy.wait()
    own_w.wait()
    own_shard.wait()

    shard_up.wait_recv()
    go(shard_on)
    forth(0).wait_recv()
    go(again(0))
    go(forth(3))
    go(twin_near(0))
    back(1).wait_recv()
    go(over(1))
    go(back(4))
    shard_down.wait_recv()
    shard_on.wait_recv()
    go(rise(0))
    go(sink(0))
    go(share(0))
    twin_near(0).wait_recv()
    first_keys(0)
    forth(1).wait_recv()
    go(forth(2))
    go(twin_near(1))
    back(2).wait_recv()
    go(over(2))
    go(back(5))
    twin_near(1).wait_recv()
    first_keys(1)
    again(0).wait_recv()
    go(twin_far(0))
    over(1).wait_recv()
    go(twin_far(1))
    twin_far(0).wait_recv()
    last_keys(0)
    twin_far(1).wait_recv()
    last_keys(1)
    w_right.wait_recv()
    go(w_twin_l)
    w_left.wait_recv()
    go(w_twin_r)
    w_far_r.wait_recv()
    go(w_on_r)
    w_far_l.wait_recv()
    go(w_on_l)
    rise(0).wait_recv()
    go(rise(1))
    go(share(-1))
    sink(0).wait_recv()
    go(sink(1))
    go(share(1))
    forth(3).wait_recv()
    go(again(3))
    go(forth(4))
    go(forth(5))
    go(twin_near(3))
    back(4).wait_recv()
    go(over(4))
    forth(2).wait_recv()
    go(twin_near(2))
    over(2).wait_recv()
    go(twin_far(2))
    twin_near(2).wait_recv()
    first_keys(2)
    twin_far(2).wait_recv()
    last_keys(2)
    w_on_r.wait_recv()
    w_on_l.wait_recv()
    go(w_twin_f)
    pass_context(0)
    pass_context(1)
    rise(1).wait_recv()
    go(rise(2))
    go(share(-2))
    sink(1).wait_recv()
    go(sink(2))
    go(share(2))
    twin_near(3).wait_recv()
    first_keys(3)
    back(5).wait_recv()
    go(over(5))
    again(3).wait_recv()
    go(twin_far(3))
    twin_far(3).wait_recv()
    last_keys(3)
    pass_context(2)
    forth(4).wait_recv()
    go(twin_near(4))
    twin_near(4).wait_recv()
    first_keys(4)
    over(4).wait_recv()
    go(twin_far(4))
    twin_far(4).wait_recv()
    last_keys(4)
    pass_context(3)
    rise(2).wait_recv()
    go(rise(3))
    go(share(-3))
    sink(2).wait_recv()
    go(share(3))
    forth(5).wait_recv()
    go(twin_near(5))
    twin_near(5).wait_recv()
    first_keys(5)
    over(5).wait_recv()
    go(twin_far(5))
    twin_far(5).wait_recv()
    last_keys(5)
    pass_context(4)
    for copy in (w_twin_l, w_twin_r, w_twin_f):
        copy.wait_recv()
    for h in range(4):
        ctx_on_right(h).wait_recv()
        ctx_on_left(h).wait_recv()

    def project(first, count, seed, store):
        def tile(t, carry):
            rows = pl.ds(pl.multiple_of(t * TILE, TILE), TILE)
            total = seed(rows)
            for block in range(4):
                at = block * WIDTH + first
                total = total + jnp.dot(
                    ctx[rows, at:at + count], woc[at:at + count, :], preferred_element_type=F32
                )
            store(rows, total)
            return carry

        lax.fori_loop(0, ROWS // TILE, tile, 0)

    def keep(rows, total):
        acc[rows, :] = total

    def finish(rows, total):
        hidden_ref[rows, :] = (res_ref[rows, :].astype(F32) + total).astype(BF16)

    project(0, 4 * HEAD_DIM, lambda rows: jnp.zeros((TILE, WIDTH), F32), keep)
    pass_context(5)
    for h in (4, 5):
        ctx_on_right(h).wait_recv()
        ctx_on_left(h).wait_recv()
    project(4 * HEAD_DIM, 2 * HEAD_DIM, lambda rows: acc[rows, :], finish)
    rise(3).wait_recv()
    go(share(-4))
    for steps in range(-4, 4):
        share(steps).wait_recv()
    for copy in started:
        copy.wait_send()
    assert len(copies.made) == N_SELF


N_SELF = 79


def self_layer(doc, tail, q, res, shard, k, v, wo):
    any_spec = pl.BlockSpec(memory_space=pl.ANY)
    vmem = pl.BlockSpec(memory_space=pltpu.VMEM)
    smem = pl.BlockSpec(memory_space=pltpu.SMEM)
    return pl.pallas_call(
        self_kernel,
        out_shape=(
            jax.ShapeDtypeStruct((ROWS, WIDTH), BF16),
            jax.ShapeDtypeStruct((GROUPS, 4, 2, SHARD, COLS), BF16),
        ),
        in_specs=[smem, smem, vmem, vmem, vmem, any_spec, any_spec, any_spec],
        out_specs=(vmem, any_spec),
        scratch_shapes=[
            pltpu.VMEM((SLOTS, HEADS, 2, ROWS, HEAD_DIM), BF16),
            pltpu.VMEM((len(MINUS), 2, ROWS, HEAD_DIM), BF16),
            pltpu.VMEM((ROWS, D), BF16),
            pltpu.VMEM((D, WIDTH), BF16),
            pltpu.VMEM((2, HALF // 2, WIDTH), BF16),
            pltpu.VMEM((ROWS, WIDTH), F32),
            *STATE,
            pltpu.SemaphoreType.DMA((2 * HEADS + 2,)),
            pltpu.SemaphoreType.DMA((N_SELF,)),
            pltpu.SemaphoreType.DMA((N_SELF,)),
        ],
        compiler_params=pltpu.CompilerParams(
            collective_id=0, has_side_effects=True, vmem_limit_bytes=56 * 1024 * 1024
        ),
        cost_estimate=pl.CostEstimate(
            flops=60_000_000_000, bytes_accessed=20_000_000, transcendentals=0
        ),
        name="self_layer",
    )(doc, tail, q, res, shard, k, v, wo)


PARTS = ROWS // TILE
CACHE = 2 * 2 * HEAD_DIM
CACHE_PLUS = (0, 2)
CACHE_MINUS = (1, 3)


def cross_kernel(
    doc_ref, tail_ref, gain_ref, hidden_hbm, wall_hbm, out_ref,
    hid, wall, cache, relay, queries, peak_ref, total_ref, blended_ref, local_sem, send_sem, recv_sem,
):
    refs = (peak_ref, total_ref, blended_ref)
    here = Place()
    i, x, c = here.i, here.x, here.c
    copies = Copies(send_sem, recv_sem)
    started = []
    left_x, right_x = (x + 3) % 4, (x + 1) % 4

    def cols(block):
        return pl.ds(pl.multiple_of(block * WIDTH, WIDTH), WIDTH)

    own = pltpu.make_async_copy(hidden_hbm, hid.at[:, cols(x)], local_sem.at[0])
    own.start()
    load = pltpu.make_async_copy(wall_hbm, wall, local_sem.at[1])
    load.start()
    greet([
        here.next_chip, here.prev_chip, here.relay_to, here.relay_from, here.pass_to, here.pass_from,
        here.partner, here.right, here.left,
    ])

    def go(copy):
        copy.start()
        started.append(copy)

    def rows(r):
        return pl.ds(r * TILE, TILE)

    def to_right(r):
        part = hid.at[rows(r), cols(x)]
        return copies.make(("r", r), part, part, here.right)

    def to_left(r):
        part = hid.at[rows(r), cols(x)]
        return copies.make(("l", r), part, part, here.left)

    def on_right(r):
        part = hid.at[pl.ds(r * TILE, TILE // 2), cols(left_x)]
        return copies.make(("or", r), part, part, here.right)

    def on_left(r):
        part = hid.at[pl.ds(r * TILE + TILE // 2, TILE // 2), cols(right_x)]
        return copies.make(("ol", r), part, part, here.left)

    def forth(r):
        return copies.make(("forth", r), cache.at[4, rows(r)], cache.at[1, rows(r)], here.next_chip)

    def again(r):
        return copies.make(("again", r), cache.at[1, rows(r)], cache.at[3, rows(r)], here.next_chip)

    def back(r):
        return copies.make(("back", r), cache.at[4, rows(r)], relay.at[CACHE_MINUS.index(r)], here.relay_to)

    def over(r):
        return copies.make(("over", r), relay.at[CACHE_MINUS.index(r)], cache.at[3, rows(r)], here.pass_to)

    def twin_near(r):
        return copies.make(("near", r), cache.at[1, rows(r)], cache.at[2 * (1 - c), rows(r)], here.partner)

    def twin_far(r):
        return copies.make(("far", r), cache.at[4 - c, rows(r)], cache.at[2 * c, rows(r)], here.partner)

    def hand_on(r):
        to_right(r).wait_recv()
        go(on_right(r))
        to_left(r).wait_recv()
        go(on_left(r))

    def make_part(r):
        on_right(r).wait_recv()
        on_left(r).wait_recv()
        wide = hid[r * TILE:(r + 1) * TILE, :].astype(F32)
        mean_square = jnp.sum(wide * wide, axis=1, keepdims=True) / D
        normed = (wide * lax.rsqrt(mean_square + EPSILON) * gain_ref[...]).astype(BF16)
        made = jnp.dot(normed, wall[:, WIDTH:], preferred_element_type=F32).astype(BF16)
        cache[4, r * TILE:(r + 1) * TILE, :] = made
        asked = jnp.dot(normed, wall[:, :WIDTH], preferred_element_type=F32).astype(BF16)
        queries[r * TILE:(r + 1) * TILE, :] = asked
        go(forth(r))
        if r in CACHE_MINUS:
            go(back(r))

    def arrive(r):
        forth(r).wait_recv()
        go(twin_near(r))
        if r in CACHE_PLUS:
            go(again(r))
        else:
            back(r).wait_recv()
            go(over(r))

    def finish(r):
        (again if r in CACHE_PLUS else over)(r).wait_recv()
        go(twin_far(r))

    own.wait()
    for r in (0, 1):
        go(to_right(r))
        go(to_left(r))
    hand_on(0)
    go(to_right(2))
    go(to_left(2))
    load.wait()
    hand_on(1)
    go(to_right(3))
    go(to_left(3))
    make_part(0)
    hand_on(2)
    make_part(1)
    arrive(0)
    hand_on(3)
    make_part(2)
    arrive(1)
    finish(0)
    make_part(3)
    arrive(2)
    finish(1)

    limits = key_limits(doc_ref, tail_ref, i)
    near_limit = jnp.where(c == 0, limits[1], limits[3])
    far_limit = jnp.where(c == 0, limits[3], limits[1])

    def head_cols(h):
        return pl.ds(pl.multiple_of(h * HEAD_DIM, HEAD_DIM), HEAD_DIM)

    def step(h, slot, limit, state, past=None):
        g = h // 3
        return flash_step(
            queries[:, head_cols(h)],
            cache[slot, :, head_cols(g)],
            cache[slot, :, head_cols(g + 2)],
            limit, state, past,
        )

    def own_keys(h, carry):
        put_state(refs, h, step(h, 4, limits[0], None, "own"))
        return carry

    lax.fori_loop(0, HEADS, own_keys, 0)
    arrive(3)
    finish(2)
    for r in range(PARTS):
        twin_near(r).wait_recv()

    def near_keys(h, carry):
        state = step(h, 1, limits[2], get_state(refs, h))
        put_state(refs, h, step(h, 2 * c, near_limit, state))
        return carry

    lax.fori_loop(0, HEADS, near_keys, 0)
    finish(3)
    for r in range(PARTS):
        twin_far(r).wait_recv()

    def far_keys(h, carry):
        state = step(h, 3, limits[4], get_state(refs, h))
        state = step(h, 2 * (1 - c), far_limit, state)
        out_ref[:, head_cols(h)] = (state[2] / state[1]).astype(BF16)
        return carry

    lax.fori_loop(0, HEADS, far_keys, 0)
    for copy in started:
        copy.wait_send()
    assert len(copies.made) == N_CROSS


N_CROSS = 34


def cross_layer(doc, tail, gain, hidden, wall):
    any_spec = pl.BlockSpec(memory_space=pl.ANY)
    vmem = pl.BlockSpec(memory_space=pltpu.VMEM)
    smem = pl.BlockSpec(memory_space=pltpu.SMEM)
    return pl.pallas_call(
        cross_kernel,
        out_shape=jax.ShapeDtypeStruct((ROWS, WIDTH), BF16),
        in_specs=[smem, smem, vmem, any_spec, any_spec],
        out_specs=vmem,
        scratch_shapes=[
            pltpu.VMEM((ROWS, D), BF16),
            pltpu.VMEM((D, COLS), BF16),
            pltpu.VMEM((SLOTS, ROWS, CACHE), BF16),
            pltpu.VMEM((len(CACHE_MINUS), TILE, CACHE), BF16),
            pltpu.VMEM((ROWS, WIDTH), BF16),
            *STATE,
            pltpu.SemaphoreType.DMA((2,)),
            pltpu.SemaphoreType.DMA((N_CROSS,)),
            pltpu.SemaphoreType.DMA((N_CROSS,)),
        ],
        compiler_params=pltpu.CompilerParams(
            collective_id=1, has_side_effects=True, vmem_limit_bytes=56 * 1024 * 1024
        ),
        cost_estimate=pl.CostEstimate(
            flops=60_000_000_000, bytes_accessed=20_000_000, transcendentals=0
        ),
        name="cross_layer",
    )(doc, tail, gain, hidden, wall)


def local(
    residual, q_self, k_self, v_self, w_out, norm_gain, w_query, w_cache, block_doc, tail_len
):
    shard = jnp.concatenate([w_query, w_cache], axis=1)
    hidden, wall = self_layer(
        block_doc, tail_len, q_self, residual, shard, k_self, v_self, w_out
    )
    cross = cross_layer(
        block_doc, tail_len, norm_gain.reshape(1, D), hidden, wall.reshape(D, COLS)
    )
    return (hidden, cross)


def solution(mesh):
    in_specs = (
        P("seq", "head"),
        P("seq", "head"),
        P("seq", "head"),
        P("seq", "head"),
        P("head", None),
        P(),
        P("seq", "head"),
        P("seq", "head"),
        P(),
        P(),
    )
    out_specs = (P("seq", "head"), P("seq", "head"))
    return jax.shard_map(local, mesh=mesh, in_specs=in_specs, out_specs=out_specs, check_vma=False)
```

```python
import functools
import math

import jax
import jax.numpy as jnp
from jax import lax
from jax.experimental import pallas as pl
from jax.experimental.pallas import tpu as pltpu
from jax.sharding import PartitionSpec as P

D = 3072
HEAD_DIM = 128
ROWS = 512
NBLK = 64
HEADS = 6
SLOTS = 5
WIDTH = HEADS * HEAD_DIM
HALF = WIDTH // 2
EPSILON = 1e-06
SCALE = 1.0 / math.sqrt(HEAD_DIM)
EXP2_SCALE = SCALE * math.log2(math.e)
MASKED = -1e30
LARGE = 3.0e38
TILE = 128
GROUPS = 8
SHARD = D // NBLK
COLS = WIDTH + 2 * 2 * HEAD_DIM

MESH = pl.DeviceIdType.MESH
F32 = jnp.float32
BF16 = jnp.bfloat16

PLUS = (0, 3)
MINUS = (1, 2, 4, 5)


PARTS = ROWS // TILE
CACHE = 2 * 2 * HEAD_DIM
CACHE_PLUS = (0, 2)
CACHE_MINUS = (1, 3)


class Copies:
    def __init__(self, send_sem, recv_sem):
        self.send_sem, self.recv_sem = send_sem, recv_sem
        self.made = {}

    def make(self, name, src, dst, device):
        if name not in self.made:
            self.made[name] = len(self.made)
        n = self.made[name]
        return pltpu.make_async_remote_copy(
            src_ref=src,
            dst_ref=dst,
            send_sem=self.send_sem.at[n],
            recv_sem=self.recv_sem.at[n],
            device_id=device,
            device_id_type=MESH,
        )


class Place:
    def __init__(self):
        i = lax.axis_index("seq")
        x = lax.axis_index("head")
        self.i, self.x = i, x
        c = i % 2
        y = (i // 2) % 4
        z = i // 8
        self.c, self.y, self.z = c, y, z

        def at(zz, yy, cc):
            return ((zz + 8) % 8 * 4 + yy) * 2 + cc

        up = (y + 1) % 4
        down = (y + 3) % 4
        self.next_chip = (at(z + (y + 1) // 4, up, c), x)
        self.prev_chip = (at(z - (6 - y) // 6, down, c), x)
        self.relay_to = (at(z, down, c), x)
        self.relay_from = (at(z, up, c), x)
        self.pass_to = (at(z + (up + 2) // 4, down, c), x)
        self.pass_from = (at(z - ((y + 2) % 4) // 2, up, c), x)
        self.partner = (i + 1 - 2 * c, x)
        self.right = (i, (x + 1) % 4)
        self.left = (i, (x + 3) % 4)
        self.y_up, self.y_down = (at(z, up, c), x), (at(z, down, c), x)
        self.y_far = (at(z, (y + 2) % 4, c), x)
        self.z_up, self.z_down = (at(z + 1, y, c), x), (at(z - 1, y, c), x)


def greet(devices):
    barrier = pltpu.get_barrier_semaphore()
    for device in devices:
        pl.semaphore_signal(barrier, inc=1, device_id=device, device_id_type=MESH)
    pl.semaphore_wait(barrier, len(devices))


def key_limits(doc_ref, tail_ref, i):
    limits = []
    own = doc_ref[i]
    for d in range(SLOTS):
        j = jnp.maximum(i - d, 0)
        doc = doc_ref[j]
        after = doc_ref[jnp.minimum(j + 1, NBLK - 1)]
        closing = jnp.logical_or(j == NBLK - 1, after != doc)
        count = jnp.where(closing, tail_ref[j], ROWS)
        seen = jnp.logical_and(i - d >= 0, doc == own)
        limits.append(jnp.where(seen, count, 0))
    return limits


def flash_step(q, keys, values, limit, state, past=None):
    rows = q.shape[0]
    lane = lax.broadcasted_iota(jnp.int32, (1, ROWS), 1)
    s = lax.dot_general(q, keys, (((1,), (1,)), ((), ())), preferred_element_type=F32)
    s = jnp.minimum(s, jnp.where(lane < limit, LARGE, MASKED))
    if past is not None:
        query_at = lax.broadcasted_iota(jnp.int32, (rows, ROWS), 0)
        key_at = lax.broadcasted_iota(jnp.int32, (rows, ROWS), 1)
        s = jnp.where(key_at <= query_at if past == "own" else key_at > query_at, s, MASKED)
    peak = jnp.max(s, axis=1, keepdims=True)
    if state is not None:
        peak = jnp.maximum(peak, state[0])
    spread = peak if peak.shape[1] == 1 else jnp.concatenate([peak] * (ROWS // HEAD_DIM), axis=1)
    weights = jnp.exp2((s - spread) * EXP2_SCALE)
    total = jnp.sum(weights, axis=1, keepdims=True)
    blended = jnp.dot(weights.astype(BF16), values, preferred_element_type=F32)
    if state is not None:
        shrink = jnp.exp2((state[0] - peak) * EXP2_SCALE)
        total = state[1] * shrink + total
        blended = state[2] * shrink + blended
    return peak, total, blended


def put_state(refs, h, state):
    peak_ref, total_ref, blended_ref = refs
    peak_ref[h] = jnp.broadcast_to(state[0], (ROWS, HEAD_DIM))
    total_ref[h] = jnp.broadcast_to(state[1], (ROWS, HEAD_DIM))
    blended_ref[h] = state[2]


def get_state(refs, h):
    peak_ref, total_ref, blended_ref = refs
    return peak_ref[h], total_ref[h], blended_ref[h]


STATE = [
    pltpu.VMEM((HEADS, ROWS, HEAD_DIM), F32),
    pltpu.VMEM((HEADS, ROWS, HEAD_DIM), F32),
    pltpu.VMEM((HEADS, ROWS, HEAD_DIM), F32),
]


def layer_kernel(
    doc_ref, tail_ref, q_ref, res_ref, gain_ref, k_hbm, v_hbm, wo_hbm, wq_hbm, wc_hbm,
    hidden_ref, out_ref,
    kv, relay, ctx, woc, wrelay, acc, peak_ref, total_ref, blended_ref,
    hid, wall, cache, crelay, queries, local_sem, send_sem, recv_sem,
):
    refs = (peak_ref, total_ref, blended_ref)
    here = Place()
    i, x, c = here.i, here.x, here.c
    copies = Copies(send_sem, recv_sem)
    started = []
    right_x, left_x, far_x = (x + 1) % 4, (x + 3) % 4, (x + 2) % 4

    local = []
    for h in range(HEADS):
        cols = pl.ds(h * HEAD_DIM, HEAD_DIM)
        one = pltpu.make_async_copy(k_hbm.at[:, cols], kv.at[SLOTS - 1, h, 0], local_sem.at[2 * h])
        two = pltpu.make_async_copy(v_hbm.at[:, cols], kv.at[SLOTS - 1, h, 1], local_sem.at[2 * h + 1])
        one.start()
        two.start()
        local.append((one, two))
    own_rows = pl.ds(pl.multiple_of(x * WIDTH, WIDTH), WIDTH)
    own_cols = pl.ds(pl.multiple_of(x * WIDTH, WIDTH), WIDTH)
    own_w = pltpu.make_async_copy(wo_hbm.at[:, own_cols], woc.at[own_rows], local_sem.at[2 * HEADS])
    own_w.start()
    shard = wall.at[here.z, here.y, c]
    shard_loads = (
        pltpu.make_async_copy(wq_hbm, shard.at[:, pl.ds(0, WIDTH)], local_sem.at[2 * HEADS + 1]),
        pltpu.make_async_copy(wc_hbm, shard.at[:, pl.ds(WIDTH, CACHE)], local_sem.at[2 * HEADS + 2]),
    )
    for copy in shard_loads:
        copy.start()

    greet([
        here.next_chip, here.prev_chip, here.relay_to, here.relay_from, here.pass_to, here.pass_from,
        here.partner, here.right, here.left, here.y_up, here.y_down, here.y_far, here.y_far, here.z_up, here.z_down,
    ])

    def go(copy):
        copy.start()
        started.append(copy)

    shard_up = copies.make("su", shard, shard, here.y_up)
    shard_down = copies.make("sd", shard, shard, here.y_down)
    shard_far = copies.make("sf", shard, shard, here.y_far)

    def group(steps, part):
        return wall.at[(here.z + GROUPS + steps) % GROUPS, pl.ds(2 * part, 2), c]

    def rise(n, part):
        return copies.make(("rise", n, part), group(-n, part), group(-n, part), here.z_up)

    def sink(n, part):
        return copies.make(("sink", n, part), group(n, part), group(n, part), here.z_down)

    def share(steps, part):
        return copies.make(("share", steps, part), group(steps, part), group(steps, part), here.partner)

    def forth(h):
        return copies.make(("forth", h), kv.at[4, h], kv.at[1, h], here.next_chip)

    def again(h):
        return copies.make(("again", h), kv.at[1, h], kv.at[3, h], here.next_chip)

    def back(h):
        return copies.make(("back", h), kv.at[4, h], relay.at[MINUS.index(h)], here.relay_to)

    def over(h):
        return copies.make(("over", h), relay.at[MINUS.index(h)], kv.at[3, h], here.pass_to)

    def twin_near(h):
        return copies.make(("near", h), kv.at[1, h], kv.at[2 * (1 - c), h], here.partner)

    def twin_far(h):
        return copies.make(("far", h), kv.at[4 - c, h], kv.at[2 * c, h], here.partner)

    def w_rows(block, first, count):
        return pl.ds(pl.multiple_of(block * WIDTH + c * HALF + first, 64), count)

    def w_cols(block):
        return pl.ds(pl.multiple_of(block * WIDTH, WIDTH), WIDTH)

    quarter = HALF // 2
    c_half = pl.ds(pl.multiple_of(c * HALF, HALF), HALF)
    c_one = pl.ds(pl.multiple_of(c * HALF, 64), quarter)
    c_two = pl.ds(pl.multiple_of(c * HALF + quarter, 64), quarter)
    w_right = copies.make("wr", wo_hbm.at[c_half, w_cols(right_x)], woc.at[w_rows(x, 0, HALF)], here.right)
    w_left = copies.make("wl", wo_hbm.at[c_half, w_cols(left_x)], woc.at[w_rows(x, 0, HALF)], here.left)
    w_far_r = copies.make("wfr", wo_hbm.at[c_one, w_cols(far_x)], wrelay.at[0], here.right)
    w_far_l = copies.make("wfl", wo_hbm.at[c_two, w_cols(far_x)], wrelay.at[1], here.left)
    w_on_r = copies.make("wor", wrelay.at[0], woc.at[w_rows(left_x, 0, quarter)], here.right)
    w_on_l = copies.make("wol", wrelay.at[1], woc.at[w_rows(right_x, quarter, quarter)], here.left)

    def w_twin(name, block):
        rows = w_rows(block, 0, HALF)
        return copies.make(("wt", name), woc.at[rows], woc.at[rows], here.partner)

    w_twin_l = w_twin("l", left_x)
    w_twin_r = w_twin("r", right_x)
    w_twin_f = w_twin("f", far_x)

    def ctx_cols(block, h):
        return pl.ds(pl.multiple_of(block * WIDTH + h * HEAD_DIM, HEAD_DIM), HEAD_DIM)

    upper, lower = pl.ds(0, ROWS // 2), pl.ds(ROWS // 2, ROWS // 2)

    def ctx_right(h):
        return copies.make(("cr", h), ctx.at[:, ctx_cols(x, h)], ctx.at[:, ctx_cols(x, h)], here.right)

    def ctx_left(h):
        return copies.make(("cl", h), ctx.at[:, ctx_cols(x, h)], ctx.at[:, ctx_cols(x, h)], here.left)

    def ctx_on_right(h):
        part = ctx.at[upper, ctx_cols(left_x, h)]
        return copies.make(("cor", h), part, part, here.right)

    def ctx_on_left(h):
        part = ctx.at[lower, ctx_cols(right_x, h)]
        return copies.make(("col", h), part, part, here.left)

    limits = key_limits(doc_ref, tail_ref, i)

    near_limit = jnp.where(c == 0, limits[1], limits[3])
    far_limit = jnp.where(c == 0, limits[3], limits[1])

    def first_keys(h):
        q = q_ref[:, h * HEAD_DIM:(h + 1) * HEAD_DIM]
        state = flash_step(q, kv[4, h, 0], kv[4, h, 1], limits[0], None, "own")
        state = flash_step(q, kv[1, h, 0], kv[1, h, 1], limits[2], state)
        near = 2 * c
        state = flash_step(q, kv[near, h, 0], kv[near, h, 1], near_limit, state)
        put_state(refs, h, state)

    def last_keys(h):
        q = q_ref[:, h * HEAD_DIM:(h + 1) * HEAD_DIM]
        state = get_state(refs, h)
        state = flash_step(q, kv[3, h, 0], kv[3, h, 1], limits[4], state, "edge")
        far = 2 * (1 - c)
        state = flash_step(q, kv[far, h, 0], kv[far, h, 1], far_limit, state)
        ctx[:, ctx_cols(x, h)] = (state[2] / state[1]).astype(BF16)
        go(ctx_right(h))
        go(ctx_left(h))

    def pass_context(h):
        ctx_right(h).wait_recv()
        go(ctx_on_right(h))
        ctx_left(h).wait_recv()
        go(ctx_on_left(h))

    def sunk(n, part, last=False):
        sink(n, part).wait_recv()
        if not last:
            go(sink(n + 1, part))
        go(share(n + 1, part))

    def risen(n, part, last=False):
        rise(n, part).wait_recv()
        if not last:
            go(rise(n + 1, part))
        go(share(-n - 1, part))

    for copy in shard_loads:
        copy.wait()
    go(shard_up)
    go(shard_down)
    go(shard_far)
    for h in (0, 1, 2):
        for copy in local[h]:
            copy.wait()
    go(forth(0))
    go(back(1))
    go(w_right)
    go(w_left)
    go(w_far_r)
    go(w_far_l)
    go(forth(1))
    go(back(2))
    for h in (3, 4, 5):
        for copy in local[h]:
            copy.wait()
    own_w.wait()

    shard_up.wait_recv()
    shard_down.wait_recv()
    shard_far.wait_recv()
    for part in (0, 1):
        go(sink(0, part))
        go(share(0, part))
    back(1).wait_recv()
    go(over(1))
    go(back(4))
    forth(0).wait_recv()
    go(again(0))
    go(forth(3))
    go(twin_near(0))
    twin_near(0).wait_recv()
    first_keys(0)
    sunk(0, 0)
    back(2).wait_recv()
    go(over(2))
    go(back(5))
    forth(1).wait_recv()
    go(forth(2))
    go(twin_near(1))
    twin_near(1).wait_recv()
    first_keys(1)
    sunk(0, 1)
    w_right.wait_recv()
    go(w_twin_l)
    w_left.wait_recv()
    go(w_twin_r)
    w_far_r.wait_recv()
    go(w_on_r)
    w_far_l.wait_recv()
    go(w_on_l)
    over(1).wait_recv()
    go(twin_far(1))
    again(0).wait_recv()
    go(twin_far(0))
    twin_far(1).wait_recv()
    last_keys(1)
    twin_far(0).wait_recv()
    last_keys(0)
    sunk(1, 0)
    back(4).wait_recv()
    go(over(4))
    forth(3).wait_recv()
    go(again(3))
    go(forth(4))
    go(forth(5))
    go(twin_near(3))
    sunk(1, 1)
    w_on_r.wait_recv()
    w_on_l.wait_recv()
    go(w_twin_f)
    twin_near(3).wait_recv()
    first_keys(3)
    over(2).wait_recv()
    go(twin_far(2))
    forth(2).wait_recv()
    go(twin_near(2))
    pass_context(1)
    pass_context(0)
    twin_near(2).wait_recv()
    first_keys(2)
    twin_far(2).wait_recv()
    last_keys(2)
    back(5).wait_recv()
    go(over(5))
    sunk(2, 0)
    again(3).wait_recv()
    go(twin_far(3))
    sunk(2, 1)
    twin_far(3).wait_recv()
    last_keys(3)
    pass_context(2)
    over(4).wait_recv()
    go(twin_far(4))
    forth(4).wait_recv()
    go(twin_near(4))
    for part in (0, 1):
        go(rise(0, part))
    twin_near(4).wait_recv()
    first_keys(4)
    twin_far(4).wait_recv()
    last_keys(4)
    sunk(3, 0)
    pass_context(3)
    over(5).wait_recv()
    go(twin_far(5))
    forth(5).wait_recv()
    go(twin_near(5))
    twin_near(5).wait_recv()
    first_keys(5)
    twin_far(5).wait_recv()
    last_keys(5)
    sunk(3, 1)
    pass_context(4)
    for copy in (w_twin_l, w_twin_r, w_twin_f):
        copy.wait_recv()
    for h in range(4):
        ctx_on_right(h).wait_recv()
        ctx_on_left(h).wait_recv()

    def project(first, count, seed, store):
        def tile(t, carry):
            rows = pl.ds(pl.multiple_of(t * TILE, TILE), TILE)
            total = seed(rows)
            for block in range(4):
                at = block * WIDTH + first
                total = total + jnp.dot(
                    ctx[rows, at:at + count], woc[at:at + count, :], preferred_element_type=F32
                )
            store(rows, total)
            return carry

        lax.fori_loop(0, ROWS // TILE, tile, 0)

    def keep(rows, total):
        acc[rows, :] = total

    def cols(block):
        return pl.ds(pl.multiple_of(block * WIDTH, WIDTH), WIDTH)

    def finish(rows, total):
        tile = (res_ref[rows, :].astype(F32) + total).astype(BF16)
        hidden_ref[rows, :] = tile
        hid[rows, cols(x)] = tile

    project(0, 4 * HEAD_DIM, lambda rows: jnp.zeros((TILE, WIDTH), F32), keep)
    pass_context(5)
    for h in (4, 5):
        ctx_on_right(h).wait_recv()
        ctx_on_left(h).wait_recv()
    project(4 * HEAD_DIM, 2 * HEAD_DIM, lambda rows: acc[rows, :], finish)

    def part_rows(r):
        return pl.ds(r * TILE, TILE)

    def to_right(r):
        part = hid.at[part_rows(r), cols(x)]
        return copies.make(("r", r), part, part, here.right)

    def to_left(r):
        part = hid.at[part_rows(r), cols(x)]
        return copies.make(("l", r), part, part, here.left)

    def on_right(r):
        part = hid.at[pl.ds(r * TILE, TILE // 2), cols(left_x)]
        return copies.make(("or", r), part, part, here.right)

    def on_left(r):
        part = hid.at[pl.ds(r * TILE + TILE // 2, TILE // 2), cols(right_x)]
        return copies.make(("ol", r), part, part, here.left)

    def c_forth(r):
        return copies.make(("c_forth", r), cache.at[4, part_rows(r)], cache.at[1, part_rows(r)], here.next_chip)

    def c_again(r):
        return copies.make(("c_again", r), cache.at[1, part_rows(r)], cache.at[3, part_rows(r)], here.next_chip)

    def c_back(r):
        return copies.make(("c_back", r), cache.at[4, part_rows(r)], crelay.at[CACHE_MINUS.index(r)], here.relay_to)

    def c_over(r):
        return copies.make(("c_over", r), crelay.at[CACHE_MINUS.index(r)], cache.at[3, part_rows(r)], here.pass_to)

    def c_near(r):
        return copies.make(("c_near", r), cache.at[1, part_rows(r)], cache.at[2 * (1 - c), part_rows(r)], here.partner)

    def c_far(r):
        return copies.make(("c_far", r), cache.at[4 - c, part_rows(r)], cache.at[2 * c, part_rows(r)], here.partner)

    def hand_on(r):
        to_right(r).wait_recv()
        go(on_right(r))
        to_left(r).wait_recv()
        go(on_left(r))

    def make_part(r):
        on_right(r).wait_recv()
        on_left(r).wait_recv()
        wide = hid[r * TILE:(r + 1) * TILE, :].astype(F32)
        mean_square = jnp.sum(wide * wide, axis=1, keepdims=True) / D
        normed = (wide * lax.rsqrt(mean_square + EPSILON) * gain_ref[...]).astype(BF16)
        made = jnp.dot(normed, wall[:, :, :, :, WIDTH:].reshape(D, CACHE), preferred_element_type=F32).astype(BF16)
        cache[4, r * TILE:(r + 1) * TILE, :] = made
        asked = jnp.dot(normed, wall[:, :, :, :, :WIDTH].reshape(D, WIDTH), preferred_element_type=F32).astype(BF16)
        queries[r * TILE:(r + 1) * TILE, :] = asked
        go(c_forth(r))
        if r in CACHE_MINUS:
            go(c_back(r))

    def c_arrive(r):
        c_forth(r).wait_recv()
        go(c_near(r))
        if r in CACHE_PLUS:
            go(c_again(r))
        else:
            c_back(r).wait_recv()
            go(c_over(r))

    def complete(r):
        (c_again if r in CACHE_PLUS else c_over)(r).wait_recv()
        go(c_far(r))

    for r in (0, 1):
        go(to_right(r))
        go(to_left(r))
    sunk(4, 0, last=True)
    risen(0, 0)
    hand_on(0)
    go(to_right(2))
    go(to_left(2))
    sunk(4, 1, last=True)
    risen(0, 1)
    hand_on(1)
    go(to_right(3))
    go(to_left(3))
    risen(1, 0, last=True)
    risen(1, 1, last=True)
    for steps in range(-2, 6):
        for part in (0, 1):
            share(steps, part).wait_recv()
    make_part(0)
    hand_on(2)
    make_part(1)
    c_arrive(0)
    hand_on(3)
    make_part(2)
    c_arrive(1)
    complete(0)
    make_part(3)
    c_arrive(2)
    complete(1)

    def head_cols(h):
        return pl.ds(pl.multiple_of(h * HEAD_DIM, HEAD_DIM), HEAD_DIM)

    def step(h, slot, limit, state, past=None):
        g = h // 3
        return flash_step(
            queries[:, head_cols(h)],
            cache[slot, :, head_cols(g)],
            cache[slot, :, head_cols(g + 2)],
            limit, state, past,
        )

    def own_keys(h, carry):
        put_state(refs, h, step(h, 4, limits[0], None, "own"))
        return carry

    lax.fori_loop(0, HEADS, own_keys, 0)
    c_arrive(3)
    complete(2)
    for r in range(PARTS):
        c_near(r).wait_recv()

    def near_keys(h, carry):
        state = step(h, 1, limits[2], get_state(refs, h))
        put_state(refs, h, step(h, 2 * c, near_limit, state))
        return carry

    lax.fori_loop(0, HEADS, near_keys, 0)
    complete(3)
    for r in range(PARTS):
        c_far(r).wait_recv()

    def far_keys(h, carry):
        state = step(h, 3, limits[4], get_state(refs, h))
        state = step(h, 2 * (1 - c), far_limit, state)
        out_ref[:, head_cols(h)] = (state[2] / state[1]).astype(BF16)
        return carry

    lax.fori_loop(0, HEADS, far_keys, 0)
    for copy in started:
        copy.wait_send()
    assert len(copies.made) == N_COPIES, len(copies.made)


N_COPIES = 61 + 3 + 10 + 4 + 16 + 34


def layer(doc, tail, q, res, gain, k, v, wo, wq, wc):
    any_spec = pl.BlockSpec(memory_space=pl.ANY)
    vmem = pl.BlockSpec(memory_space=pltpu.VMEM)
    smem = pl.BlockSpec(memory_space=pltpu.SMEM)
    return pl.pallas_call(
        layer_kernel,
        out_shape=(jax.ShapeDtypeStruct((ROWS, WIDTH), BF16),) * 2,
        in_specs=[smem, smem, vmem, vmem, vmem] + [any_spec] * 5,
        out_specs=(vmem, vmem),
        scratch_shapes=[
            pltpu.VMEM((SLOTS, HEADS, 2, ROWS, HEAD_DIM), BF16),
            pltpu.VMEM((len(MINUS), 2, ROWS, HEAD_DIM), BF16),
            pltpu.VMEM((ROWS, D), BF16),
            pltpu.VMEM((D, WIDTH), BF16),
            pltpu.VMEM((2, HALF // 2, WIDTH), BF16),
            pltpu.VMEM((ROWS, WIDTH), F32),
            *STATE,
            pltpu.VMEM((ROWS, D), BF16),
            pltpu.VMEM((GROUPS, 4, 2, SHARD, COLS), BF16),
            pltpu.VMEM((SLOTS, ROWS, CACHE), BF16),
            pltpu.VMEM((len(CACHE_MINUS), TILE, CACHE), BF16),
            pltpu.VMEM((ROWS, WIDTH), BF16),
            pltpu.SemaphoreType.DMA((2 * HEADS + 3,)),
            pltpu.SemaphoreType.DMA((N_COPIES,)),
            pltpu.SemaphoreType.DMA((N_COPIES,)),
        ],
        compiler_params=pltpu.CompilerParams(
            collective_id=0, has_side_effects=True, vmem_limit_bytes=60 * 1024 * 1024
        ),
        name="layer",
    )(doc, tail, q, res, gain, k, v, wo, wq, wc)


def local(
    residual, q_self, k_self, v_self, w_out, norm_gain, w_query, w_cache, block_doc, tail_len
):
    return layer(
        block_doc, tail_len, q_self, residual, norm_gain.reshape(1, D),
        k_self, v_self, w_out, w_query, w_cache,
    )


def solution(mesh):
    in_specs = (
        P("seq", "head"),
        P("seq", "head"),
        P("seq", "head"),
        P("seq", "head"),
        P("head", None),
        P(),
        P("seq", "head"),
        P("seq", "head"),
        P(),
        P(),
    )
    out_specs = (P("seq", "head"), P("seq", "head"))
    return jax.shard_map(local, mesh=mesh, in_specs=in_specs, out_specs=out_specs, check_vma=False)
```

```python
import functools
import math

import jax
import jax.numpy as jnp
from jax import lax
from jax.experimental import pallas as pl
from jax.experimental.pallas import tpu as pltpu
from jax.sharding import PartitionSpec as P

D = 3072
HEAD_DIM = 128
ROWS = 512
NBLK = 64
HEADS = 6
SLOTS = 5
WIDTH = HEADS * HEAD_DIM
HALF = WIDTH // 2
EPSILON = 1e-06
SCALE = 1.0 / math.sqrt(HEAD_DIM)
EXP2_SCALE = SCALE * math.log2(math.e)
MASKED = -1e30
LARGE = 3.0e38
TILE = 128
GROUPS = 8
SHARD = D // NBLK
COLS = WIDTH + 2 * 2 * HEAD_DIM

MESH = pl.DeviceIdType.MESH
F32 = jnp.float32
BF16 = jnp.bfloat16

PLUS = (0, 3)
MINUS = (1, 2, 4, 5)


PARTS = ROWS // TILE
CACHE = 2 * 2 * HEAD_DIM
CACHE_PLUS = (0, 2)
CACHE_MINUS = (1, 3)


class Copies:
    def __init__(self, send_sem, recv_sem):
        self.send_sem, self.recv_sem = send_sem, recv_sem
        self.made = {}

    def make(self, name, src, dst, device):
        if name not in self.made:
            self.made[name] = len(self.made)
        n = self.made[name]
        return pltpu.make_async_remote_copy(
            src_ref=src,
            dst_ref=dst,
            send_sem=self.send_sem.at[n],
            recv_sem=self.recv_sem.at[n],
            device_id=device,
            device_id_type=MESH,
        )


class Place:
    def __init__(self):
        i = lax.axis_index("seq")
        x = lax.axis_index("head")
        self.i, self.x = i, x
        c = i % 2
        y = (i // 2) % 4
        z = i // 8
        self.c, self.y, self.z = c, y, z

        def at(zz, yy, cc):
            return ((zz + 8) % 8 * 4 + yy) * 2 + cc

        up = (y + 1) % 4
        down = (y + 3) % 4
        self.next_chip = (at(z + (y + 1) // 4, up, c), x)
        self.prev_chip = (at(z - (6 - y) // 6, down, c), x)
        self.relay_to = (at(z, down, c), x)
        self.relay_from = (at(z, up, c), x)
        self.pass_to = (at(z + (up + 2) // 4, down, c), x)
        self.pass_from = (at(z - ((y + 2) % 4) // 2, up, c), x)
        self.partner = (i + 1 - 2 * c, x)
        self.right = (i, (x + 1) % 4)
        self.left = (i, (x + 3) % 4)
        self.across = (i, (x + 2) % 4)
        self.y_up, self.y_down = (at(z, up, c), x), (at(z, down, c), x)
        self.y_far = (at(z, (y + 2) % 4, c), x)
        self.z_up, self.z_down = (at(z + 1, y, c), x), (at(z - 1, y, c), x)


def greet(devices):
    barrier = pltpu.get_barrier_semaphore()
    for device in devices:
        pl.semaphore_signal(barrier, inc=1, device_id=device, device_id_type=MESH)
    pl.semaphore_wait(barrier, len(devices))


def key_limits(doc_ref, tail_ref, i):
    limits = []
    own = doc_ref[i]
    for d in range(SLOTS):
        j = jnp.maximum(i - d, 0)
        doc = doc_ref[j]
        after = doc_ref[jnp.minimum(j + 1, NBLK - 1)]
        closing = jnp.logical_or(j == NBLK - 1, after != doc)
        count = jnp.where(closing, tail_ref[j], ROWS)
        seen = jnp.logical_and(i - d >= 0, doc == own)
        limits.append(jnp.where(seen, count, 0))
    return limits


def flash_step(q, keys, values, limit, state, past=None):
    rows = q.shape[0]
    lane = lax.broadcasted_iota(jnp.int32, (1, ROWS), 1)
    s = lax.dot_general(q, keys, (((1,), (1,)), ((), ())), preferred_element_type=F32)
    s = jnp.minimum(s, jnp.where(lane < limit, LARGE, MASKED))
    if past is not None:
        query_at = lax.broadcasted_iota(jnp.int32, (rows, ROWS), 0)
        key_at = lax.broadcasted_iota(jnp.int32, (rows, ROWS), 1)
        s = jnp.where(key_at <= query_at if past == "own" else key_at > query_at, s, MASKED)
    peak = jnp.max(s, axis=1, keepdims=True)
    if state is not None:
        peak = jnp.maximum(peak, state[0])
    spread = peak if peak.shape[1] == 1 else jnp.concatenate([peak] * (ROWS // HEAD_DIM), axis=1)
    weights = jnp.exp2((s - spread) * EXP2_SCALE)
    total = jnp.sum(weights, axis=1, keepdims=True)
    blended = jnp.dot(weights.astype(BF16), values, preferred_element_type=F32)
    if state is not None:
        shrink = jnp.exp2((state[0] - peak) * EXP2_SCALE)
        total = state[1] * shrink + total
        blended = state[2] * shrink + blended
    return peak, total, blended


def put_state(refs, h, state):
    peak_ref, total_ref, blended_ref = refs
    peak_ref[h] = jnp.broadcast_to(state[0], (ROWS, HEAD_DIM))
    total_ref[h] = jnp.broadcast_to(state[1], (ROWS, HEAD_DIM))
    blended_ref[h] = state[2]


def get_state(refs, h):
    peak_ref, total_ref, blended_ref = refs
    return peak_ref[h], total_ref[h], blended_ref[h]


STATE = [
    pltpu.VMEM((HEADS, ROWS, HEAD_DIM), F32),
    pltpu.VMEM((HEADS, ROWS, HEAD_DIM), F32),
    pltpu.VMEM((HEADS, ROWS, HEAD_DIM), F32),
]


def layer_kernel(
    doc_ref, tail_ref, q_ref, res_ref, gain_ref, k_hbm, v_hbm, wo_hbm, wq_hbm, wc_hbm,
    hidden_ref, out_ref,
    kv, relay, ctx, woc, acc, peak_ref, total_ref, blended_ref,
    hid, wall, cache, crelay, queries, local_sem, send_sem, recv_sem, clear_sem,
):
    refs = (peak_ref, total_ref, blended_ref)
    here = Place()
    i, x, c = here.i, here.x, here.c
    copies = Copies(send_sem, recv_sem)
    started = []
    right_x, left_x, far_x = (x + 1) % 4, (x + 3) % 4, (x + 2) % 4

    local = []
    for h in range(HEADS):
        cols = pl.ds(h * HEAD_DIM, HEAD_DIM)
        one = pltpu.make_async_copy(k_hbm.at[:, cols], kv.at[SLOTS - 1, h, 0], local_sem.at[2 * h])
        two = pltpu.make_async_copy(v_hbm.at[:, cols], kv.at[SLOTS - 1, h, 1], local_sem.at[2 * h + 1])
        one.start()
        two.start()
        local.append((one, two))
    own_rows = pl.ds(pl.multiple_of(x * WIDTH, WIDTH), WIDTH)
    own_cols = pl.ds(pl.multiple_of(x * WIDTH, WIDTH), WIDTH)
    own_w = pltpu.make_async_copy(wo_hbm.at[:, own_cols], woc.at[own_rows], local_sem.at[2 * HEADS])
    own_w.start()
    shard = wall.at[here.z, here.y, c]
    shard_loads = (
        pltpu.make_async_copy(wq_hbm, shard.at[:, pl.ds(0, WIDTH)], local_sem.at[2 * HEADS + 1]),
        pltpu.make_async_copy(wc_hbm, shard.at[:, pl.ds(WIDTH, CACHE)], local_sem.at[2 * HEADS + 2]),
    )
    for copy in shard_loads:
        copy.start()

    greet([
        here.next_chip, here.prev_chip, here.relay_to, here.relay_from, here.pass_to, here.pass_from,
        here.partner, here.right, here.left, here.across, here.across, here.y_up, here.y_down, here.y_far, here.y_far, here.z_up, here.z_down,
    ])

    def go(copy):
        copy.start()
        started.append(copy)

    shard_up = copies.make("su", shard, shard, here.y_up)
    shard_down = copies.make("sd", shard, shard, here.y_down)
    shard_far = copies.make("sf", shard, shard, here.y_far)

    def group(steps, part):
        return wall.at[(here.z + GROUPS + steps) % GROUPS, pl.ds(2 * part, 2), c]

    def rise(n, part):
        return copies.make(("rise", n, part), group(-n, part), group(-n, part), here.z_up)

    def sink(n, part):
        return copies.make(("sink", n, part), group(n, part), group(n, part), here.z_down)

    def share(steps, part):
        return copies.make(("share", steps, part), group(steps, part), group(steps, part), here.partner)

    def forth(h):
        return copies.make(("forth", h), kv.at[4, h], kv.at[1, h], here.next_chip)

    def again(h):
        return copies.make(("again", h), kv.at[1, h], kv.at[3, h], here.next_chip)

    def back(h):
        return copies.make(("back", h), kv.at[4, h], relay.at[MINUS.index(h)], here.relay_to)

    def over(h):
        return copies.make(("over", h), relay.at[MINUS.index(h)], kv.at[3, h], here.pass_to)

    def twin_near(h):
        return copies.make(("near", h), kv.at[1, h], kv.at[2 * (1 - c), h], here.partner)

    def twin_far(h):
        return copies.make(("far", h), kv.at[4 - c, h], kv.at[2 * c, h], here.partner)

    def w_rows(block, first, count):
        return pl.ds(pl.multiple_of(block * WIDTH + c * HALF + first, 64), count)

    def w_cols(block):
        return pl.ds(pl.multiple_of(block * WIDTH, WIDTH), WIDTH)

    c_half = pl.ds(pl.multiple_of(c * HALF, HALF), HALF)
    w_right = copies.make("wr", wo_hbm.at[c_half, w_cols(right_x)], woc.at[w_rows(x, 0, HALF)], here.right)
    w_left = copies.make("wl", wo_hbm.at[c_half, w_cols(left_x)], woc.at[w_rows(x, 0, HALF)], here.left)
    w_far = copies.make("wf", wo_hbm.at[c_half, w_cols(far_x)], woc.at[w_rows(x, 0, HALF)], here.across)

    def w_twin(name, block):
        rows = w_rows(block, 0, HALF)
        return copies.make(("wt", name), woc.at[rows], woc.at[rows], here.partner)

    w_twin_l = w_twin("l", left_x)
    w_twin_r = w_twin("r", right_x)
    w_twin_f = w_twin("f", far_x)

    def ctx_cols(block, h):
        return pl.ds(pl.multiple_of(block * WIDTH + h * HEAD_DIM, HEAD_DIM), HEAD_DIM)

    def ctx_right(h):
        return copies.make(("cr", h), ctx.at[:, ctx_cols(x, h)], ctx.at[:, ctx_cols(x, h)], here.right)

    def ctx_left(h):
        return copies.make(("cl", h), ctx.at[:, ctx_cols(x, h)], ctx.at[:, ctx_cols(x, h)], here.left)

    def ctx_across(h):
        return copies.make(("ca", h), ctx.at[:, ctx_cols(x, h)], ctx.at[:, ctx_cols(x, h)], here.across)

    limits = key_limits(doc_ref, tail_ref, i)

    near_limit = jnp.where(c == 0, limits[1], limits[3])
    far_limit = jnp.where(c == 0, limits[3], limits[1])

    def own_keys(h):
        q = q_ref[:, h * HEAD_DIM:(h + 1) * HEAD_DIM]
        put_state(refs, h, flash_step(q, kv[4, h, 0], kv[4, h, 1], limits[0], None, "own"))

    def first_keys(h):
        q = q_ref[:, h * HEAD_DIM:(h + 1) * HEAD_DIM]
        state = flash_step(q, kv[1, h, 0], kv[1, h, 1], limits[2], get_state(refs, h))
        near = 2 * c
        state = flash_step(q, kv[near, h, 0], kv[near, h, 1], near_limit, state)
        put_state(refs, h, state)

    def last_keys(h):
        q = q_ref[:, h * HEAD_DIM:(h + 1) * HEAD_DIM]
        state = get_state(refs, h)
        state = flash_step(q, kv[3, h, 0], kv[3, h, 1], limits[4], state, "edge")
        far = 2 * (1 - c)
        state = flash_step(q, kv[far, h, 0], kv[far, h, 1], far_limit, state)
        ctx[:, ctx_cols(x, h)] = (state[2] / state[1]).astype(BF16)
        go(ctx_right(h))
        go(ctx_left(h))
        go(ctx_across(h))

    def take_context(h):
        ctx_right(h).wait_recv()
        ctx_left(h).wait_recv()
        ctx_across(h).wait_recv()

    def sunk(n, part, last=False):
        sink(n, part).wait_recv()
        if not last:
            go(sink(n + 1, part))
        go(share(n + 1, part))

    def risen(n, part, last=False):
        rise(n, part).wait_recv()
        if not last:
            go(rise(n + 1, part))
        go(share(-n - 1, part))

    for copy in shard_loads:
        copy.wait()
    shards = (shard_up, shard_down, shard_far)
    for copy in shards:
        copy.start()
    go(w_right)
    go(w_left)
    go(w_far)
    for copy in local[0] + local[1]:
        copy.wait()
    own_keys(0)
    own_keys(1)
    for h in (2, 3, 4, 5):
        for copy in local[h]:
            copy.wait()
    own_keys(2)
    for copy in shards:
        copy.wait_send()
    pl.semaphore_signal(clear_sem, inc=1, device_id=here.z_down, device_id_type=MESH)
    pl.semaphore_wait(clear_sem, 1)
    go(forth(0))
    go(back(1))
    go(forth(1))
    go(back(2))
    own_w.wait()
    for copy in shards:
        copy.wait_recv()
    for part in (0, 1):
        go(sink(0, part))
        go(share(0, part))
    for h in (3, 4, 5):
        own_keys(h)
    back(1).wait_recv()
    go(over(1))
    go(back(4))
    forth(0).wait_recv()
    go(again(0))
    go(forth(3))
    go(twin_near(0))
    twin_near(0).wait_recv()
    first_keys(0)
    sunk(0, 0)
    back(2).wait_recv()
    go(over(2))
    go(back(5))
    forth(1).wait_recv()
    go(forth(2))
    go(twin_near(1))
    twin_near(1).wait_recv()
    first_keys(1)
    sunk(0, 1)
    w_right.wait_recv()
    go(w_twin_l)
    w_left.wait_recv()
    go(w_twin_r)
    w_far.wait_recv()
    go(w_twin_f)
    over(1).wait_recv()
    go(twin_far(1))
    again(0).wait_recv()
    go(twin_far(0))
    twin_far(1).wait_recv()
    last_keys(1)
    twin_far(0).wait_recv()
    last_keys(0)
    sunk(1, 0)
    back(4).wait_recv()
    go(over(4))
    forth(3).wait_recv()
    go(again(3))
    go(forth(4))
    go(forth(5))
    go(twin_near(3))
    sunk(1, 1)
    twin_near(3).wait_recv()
    first_keys(3)
    over(2).wait_recv()
    go(twin_far(2))
    forth(2).wait_recv()
    go(twin_near(2))
    twin_near(2).wait_recv()
    first_keys(2)
    twin_far(2).wait_recv()
    last_keys(2)
    back(5).wait_recv()
    go(over(5))
    sunk(2, 0)
    again(3).wait_recv()
    go(twin_far(3))
    sunk(2, 1)
    twin_far(3).wait_recv()
    last_keys(3)
    over(4).wait_recv()
    go(twin_far(4))
    forth(4).wait_recv()
    go(twin_near(4))
    for part in (0, 1):
        go(rise(0, part))
    twin_near(4).wait_recv()
    first_keys(4)
    twin_far(4).wait_recv()
    last_keys(4)
    sunk(3, 0)
    over(5).wait_recv()
    go(twin_far(5))
    forth(5).wait_recv()
    go(twin_near(5))
    twin_near(5).wait_recv()
    first_keys(5)
    twin_far(5).wait_recv()
    last_keys(5)
    sunk(3, 1)
    for copy in (w_twin_l, w_twin_r, w_twin_f):
        copy.wait_recv()
    for h in range(4):
        take_context(h)

    def project(first, count, seed, store):
        def tile(t, carry):
            rows = pl.ds(pl.multiple_of(t * TILE, TILE), TILE)
            total = seed(rows)
            for block in range(4):
                at = block * WIDTH + first
                total = total + jnp.dot(
                    ctx[rows, at:at + count], woc[at:at + count, :], preferred_element_type=F32
                )
            store(rows, total)
            return carry

        lax.fori_loop(0, ROWS // TILE, tile, 0)

    def keep(rows, total):
        acc[rows, :] = total

    def cols(block):
        return pl.ds(pl.multiple_of(block * WIDTH, WIDTH), WIDTH)

    def finish(rows, total):
        tile = (res_ref[rows, :].astype(F32) + total).astype(BF16)
        hidden_ref[rows, :] = tile
        hid[rows, cols(x)] = tile

    project(0, 4 * HEAD_DIM, lambda rows: jnp.zeros((TILE, WIDTH), F32), keep)
    take_context(4)
    take_context(5)
    project(4 * HEAD_DIM, 2 * HEAD_DIM, lambda rows: acc[rows, :], finish)

    def part_rows(r):
        return pl.ds(r * TILE, TILE)

    def to_right(r):
        part = hid.at[part_rows(r), cols(x)]
        return copies.make(("r", r), part, part, here.right)

    def to_left(r):
        part = hid.at[part_rows(r), cols(x)]
        return copies.make(("l", r), part, part, here.left)

    def to_far(r):
        part = hid.at[part_rows(r), cols(x)]
        return copies.make(("a", r), part, part, here.across)

    def c_forth(r):
        return copies.make(("c_forth", r), cache.at[4, part_rows(r)], cache.at[1, part_rows(r)], here.next_chip)

    def c_again(r):
        return copies.make(("c_again", r), cache.at[1, part_rows(r)], cache.at[3, part_rows(r)], here.next_chip)

    def c_back(r):
        return copies.make(("c_back", r), cache.at[4, part_rows(r)], crelay.at[CACHE_MINUS.index(r)], here.relay_to)

    def c_over(r):
        return copies.make(("c_over", r), crelay.at[CACHE_MINUS.index(r)], cache.at[3, part_rows(r)], here.pass_to)

    def c_near(r):
        return copies.make(("c_near", r), cache.at[1, part_rows(r)], cache.at[2 * (1 - c), part_rows(r)], here.partner)

    def c_far(r):
        return copies.make(("c_far", r), cache.at[4 - c, part_rows(r)], cache.at[2 * c, part_rows(r)], here.partner)

    def make_part(r):
        to_right(r).wait_recv()
        to_left(r).wait_recv()
        to_far(r).wait_recv()
        wide = hid[r * TILE:(r + 1) * TILE, :].astype(F32)
        mean_square = jnp.sum(wide * wide, axis=1, keepdims=True) / D
        normed = (wide * lax.rsqrt(mean_square + EPSILON) * gain_ref[...]).astype(BF16)
        made = jnp.dot(normed, wall[:, :, :, :, WIDTH:].reshape(D, CACHE), preferred_element_type=F32).astype(BF16)
        cache[4, r * TILE:(r + 1) * TILE, :] = made
        asked = jnp.dot(normed, wall[:, :, :, :, :WIDTH].reshape(D, WIDTH), preferred_element_type=F32).astype(BF16)
        queries[r * TILE:(r + 1) * TILE, :] = asked
        go(c_forth(r))
        if r in CACHE_MINUS:
            go(c_back(r))

    def c_arrive(r):
        c_forth(r).wait_recv()
        go(c_near(r))
        if r in CACHE_PLUS:
            go(c_again(r))
        else:
            c_back(r).wait_recv()
            go(c_over(r))

    def complete(r):
        (c_again if r in CACHE_PLUS else c_over)(r).wait_recv()
        go(c_far(r))

    for r in range(PARTS):
        go(to_right(r))
        go(to_left(r))
        go(to_far(r))
    sunk(4, 0, last=True)
    risen(0, 0)
    sunk(4, 1, last=True)
    risen(0, 1)
    risen(1, 0, last=True)
    risen(1, 1, last=True)
    for steps in range(-2, 6):
        for part in (0, 1):
            share(steps, part).wait_recv()
    make_part(0)
    make_part(1)
    c_arrive(0)
    make_part(2)
    c_arrive(1)
    complete(0)
    make_part(3)
    c_arrive(2)
    complete(1)

    def head_cols(h):
        return pl.ds(pl.multiple_of(h * HEAD_DIM, HEAD_DIM), HEAD_DIM)

    def step(h, slot, limit, state, past=None):
        g = h // 3
        return flash_step(
            queries[:, head_cols(h)],
            cache[slot, :, head_cols(g)],
            cache[slot, :, head_cols(g + 2)],
            limit, state, past,
        )

    def c_own_keys(h, carry):
        put_state(refs, h, step(h, 4, limits[0], None, "own"))
        return carry

    lax.fori_loop(0, HEADS, c_own_keys, 0)
    c_arrive(3)
    complete(2)
    for r in range(PARTS):
        c_near(r).wait_recv()

    def near_keys(h, carry):
        state = step(h, 1, limits[2], get_state(refs, h))
        put_state(refs, h, step(h, 2 * c, near_limit, state))
        return carry

    lax.fori_loop(0, HEADS, near_keys, 0)
    complete(3)
    for r in range(PARTS):
        c_far(r).wait_recv()

    def far_keys(h, carry):
        state = step(h, 3, limits[4], get_state(refs, h))
        state = step(h, 2 * (1 - c), far_limit, state)
        out_ref[:, head_cols(h)] = (state[2] / state[1]).astype(BF16)
        return carry

    lax.fori_loop(0, HEADS, far_keys, 0)
    for copy in started:
        copy.wait_send()
    assert len(copies.made) == N_COPIES, len(copies.made)


N_COPIES = 28 + 6 + 18 + 3 + 10 + 4 + 16 + 12 + 18


def layer(doc, tail, q, res, gain, k, v, wo, wq, wc):
    any_spec = pl.BlockSpec(memory_space=pl.ANY)
    vmem = pl.BlockSpec(memory_space=pltpu.VMEM)
    smem = pl.BlockSpec(memory_space=pltpu.SMEM)
    return pl.pallas_call(
        layer_kernel,
        out_shape=(jax.ShapeDtypeStruct((ROWS, WIDTH), BF16),) * 2,
        in_specs=[smem, smem, vmem, vmem, vmem] + [any_spec] * 5,
        out_specs=(vmem, vmem),
        scratch_shapes=[
            pltpu.VMEM((SLOTS, HEADS, 2, ROWS, HEAD_DIM), BF16),
            pltpu.VMEM((len(MINUS), 2, ROWS, HEAD_DIM), BF16),
            pltpu.VMEM((ROWS, D), BF16),
            pltpu.VMEM((D, WIDTH), BF16),
            pltpu.VMEM((ROWS, WIDTH), F32),
            *STATE,
            pltpu.VMEM((ROWS, D), BF16),
            pltpu.VMEM((GROUPS, 4, 2, SHARD, COLS), BF16),
            pltpu.VMEM((SLOTS, ROWS, CACHE), BF16),
            pltpu.VMEM((len(CACHE_MINUS), TILE, CACHE), BF16),
            pltpu.VMEM((ROWS, WIDTH), BF16),
            pltpu.SemaphoreType.DMA((2 * HEADS + 3,)),
            pltpu.SemaphoreType.DMA((N_COPIES,)),
            pltpu.SemaphoreType.DMA((N_COPIES,)),
            pltpu.SemaphoreType.REGULAR,
        ],
        compiler_params=pltpu.CompilerParams(
            collective_id=0, has_side_effects=True, vmem_limit_bytes=60 * 1024 * 1024
        ),
        name="layer",
    )(doc, tail, q, res, gain, k, v, wo, wq, wc)


def local(
    residual, q_self, k_self, v_self, w_out, norm_gain, w_query, w_cache, block_doc, tail_len
):
    return layer(
        block_doc, tail_len, q_self, residual, norm_gain.reshape(1, D),
        k_self, v_self, w_out, w_query, w_cache,
    )


def solution(mesh):
    in_specs = (
        P("seq", "head"),
        P("seq", "head"),
        P("seq", "head"),
        P("seq", "head"),
        P("head", None),
        P(),
        P("seq", "head"),
        P("seq", "head"),
        P(),
        P(),
    )
    out_specs = (P("seq", "head"), P("seq", "head"))
    return jax.shard_map(local, mesh=mesh, in_specs=in_specs, out_specs=out_specs, check_vma=False)
```

```python
import functools
import math

import jax
import jax.numpy as jnp
from jax import lax
from jax.experimental import pallas as pl
from jax.experimental.pallas import tpu as pltpu
from jax.sharding import PartitionSpec as P

D = 3072
HEAD_DIM = 128
ROWS = 512
NBLK = 64
HEADS = 6
SLOTS = 5
WIDTH = HEADS * HEAD_DIM
HALF = WIDTH // 2
EPSILON = 1e-06
SCALE = 1.0 / math.sqrt(HEAD_DIM)
EXP2_SCALE = SCALE * math.log2(math.e)
MASKED = -1e30
LARGE = 3.0e38
TILE = 128
GROUPS = 8
SHARD = D // NBLK
COLS = WIDTH + 2 * 2 * HEAD_DIM

MESH = pl.DeviceIdType.MESH
F32 = jnp.float32
BF16 = jnp.bfloat16

PLUS = (0, 3)
MINUS = (1, 2, 4, 5)


PARTS = ROWS // TILE
CACHE = 2 * 2 * HEAD_DIM
CACHE_PLUS = (0, 2)
CACHE_MINUS = (1, 3)


class Copies:
    def __init__(self, send_sem, recv_sem):
        self.send_sem, self.recv_sem = send_sem, recv_sem
        self.made = {}

    def make(self, name, src, dst, device):
        if name not in self.made:
            self.made[name] = len(self.made)
        n = self.made[name]
        return pltpu.make_async_remote_copy(
            src_ref=src,
            dst_ref=dst,
            send_sem=self.send_sem.at[n],
            recv_sem=self.recv_sem.at[n],
            device_id=device,
            device_id_type=MESH,
        )


class Place:
    def __init__(self):
        i = lax.axis_index("seq")
        x = lax.axis_index("head")
        self.i, self.x = i, x
        c = i % 2
        y = (i // 2) % 4
        z = i // 8
        self.c, self.y, self.z = c, y, z

        def at(zz, yy, cc):
            return ((zz + 8) % 8 * 4 + yy) * 2 + cc

        up = (y + 1) % 4
        down = (y + 3) % 4
        self.next_chip = (at(z + (y + 1) // 4, up, c), x)
        self.prev_chip = (at(z - (6 - y) // 6, down, c), x)
        self.relay_to = (at(z, down, c), x)
        self.relay_from = (at(z, up, c), x)
        self.pass_to = (at(z + (up + 2) // 4, down, c), x)
        self.pass_from = (at(z - ((y + 2) % 4) // 2, up, c), x)
        self.partner = (i + 1 - 2 * c, x)
        self.right = (i, (x + 1) % 4)
        self.left = (i, (x + 3) % 4)
        self.across = (i, (x + 2) % 4)
        self.y_up, self.y_down = (at(z, up, c), x), (at(z, down, c), x)
        self.y_far = (at(z, (y + 2) % 4, c), x)
        self.z_up, self.z_down = (at(z + 1, y, c), x), (at(z - 1, y, c), x)


def greet(devices):
    barrier = pltpu.get_barrier_semaphore()
    for device in devices:
        pl.semaphore_signal(barrier, inc=1, device_id=device, device_id_type=MESH)
    pl.semaphore_wait(barrier, len(devices))


def key_limits(doc_ref, tail_ref, i):
    limits = []
    own = doc_ref[i]
    for d in range(SLOTS):
        j = jnp.maximum(i - d, 0)
        doc = doc_ref[j]
        after = doc_ref[jnp.minimum(j + 1, NBLK - 1)]
        closing = jnp.logical_or(j == NBLK - 1, after != doc)
        count = jnp.where(closing, tail_ref[j], ROWS)
        seen = jnp.logical_and(i - d >= 0, doc == own)
        limits.append(jnp.where(seen, count, 0))
    return limits


def flash_step(q, keys, values, limit, state, past=None):
    rows = q.shape[0]
    lane = lax.broadcasted_iota(jnp.int32, (1, ROWS), 1)
    s = lax.dot_general(q, keys, (((1,), (1,)), ((), ())), preferred_element_type=F32)
    s = jnp.minimum(s, jnp.where(lane < limit, LARGE, MASKED))
    if past is not None:
        query_at = lax.broadcasted_iota(jnp.int32, (rows, ROWS), 0)
        key_at = lax.broadcasted_iota(jnp.int32, (rows, ROWS), 1)
        s = jnp.where(key_at <= query_at if past == "own" else key_at > query_at, s, MASKED)
    peak = jnp.max(s, axis=1, keepdims=True)
    if state is not None:
        peak = jnp.maximum(peak, state[0])
    spread = peak if peak.shape[1] == 1 else jnp.concatenate([peak] * (ROWS // HEAD_DIM), axis=1)
    weights = jnp.exp2((s - spread) * EXP2_SCALE)
    total = jnp.sum(weights, axis=1, keepdims=True)
    blended = jnp.dot(weights.astype(BF16), values, preferred_element_type=F32)
    if state is not None:
        shrink = jnp.exp2((state[0] - peak) * EXP2_SCALE)
        total = state[1] * shrink + total
        blended = state[2] * shrink + blended
    return peak, total, blended


def put_state(refs, h, state):
    peak_ref, total_ref, blended_ref = refs
    peak_ref[h] = jnp.broadcast_to(state[0], (ROWS, HEAD_DIM))
    total_ref[h] = jnp.broadcast_to(state[1], (ROWS, HEAD_DIM))
    blended_ref[h] = state[2]


def get_state(refs, h):
    peak_ref, total_ref, blended_ref = refs
    return peak_ref[h], total_ref[h], blended_ref[h]


STATE = [
    pltpu.VMEM((HEADS, ROWS, HEAD_DIM), F32),
    pltpu.VMEM((HEADS, ROWS, HEAD_DIM), F32),
    pltpu.VMEM((HEADS, ROWS, HEAD_DIM), F32),
]


def layer_kernel(
    doc_ref, tail_ref, q_ref, res_ref, gain_ref, k_hbm, v_hbm, wo_hbm, wq_hbm, wc_hbm,
    hidden_ref, out_ref,
    kv, relay, ctx, woc, acc, peak_ref, total_ref, blended_ref,
    hid, wall, cache, crelay, queries, local_sem, send_sem, recv_sem, clear_sem,
):
    refs = (peak_ref, total_ref, blended_ref)
    here = Place()
    i, x, c = here.i, here.x, here.c
    copies = Copies(send_sem, recv_sem)
    started = []
    right_x, left_x, far_x = (x + 1) % 4, (x + 3) % 4, (x + 2) % 4

    local = []
    for h in range(HEADS):
        cols = pl.ds(h * HEAD_DIM, HEAD_DIM)
        one = pltpu.make_async_copy(k_hbm.at[:, cols], kv.at[SLOTS - 1, h, 0], local_sem.at[2 * h])
        two = pltpu.make_async_copy(v_hbm.at[:, cols], kv.at[SLOTS - 1, h, 1], local_sem.at[2 * h + 1])
        one.start()
        two.start()
        local.append((one, two))
    own_rows = pl.ds(pl.multiple_of(x * WIDTH, WIDTH), WIDTH)
    own_cols = pl.ds(pl.multiple_of(x * WIDTH, WIDTH), WIDTH)
    own_w = pltpu.make_async_copy(wo_hbm.at[:, own_cols], woc.at[own_rows], local_sem.at[2 * HEADS])
    own_w.start()
    shard = wall.at[here.z, here.y, c]
    shard_loads = (
        pltpu.make_async_copy(wq_hbm, shard.at[:, pl.ds(0, WIDTH)], local_sem.at[2 * HEADS + 1]),
        pltpu.make_async_copy(wc_hbm, shard.at[:, pl.ds(WIDTH, CACHE)], local_sem.at[2 * HEADS + 2]),
    )
    for copy in shard_loads:
        copy.start()

    greet([
        here.next_chip, here.prev_chip, here.relay_to, here.relay_from, here.pass_to, here.pass_from,
        here.partner, here.right, here.left, here.across, here.across, here.y_up, here.y_down, here.y_far, here.y_far, here.z_up, here.z_down,
    ])

    def go(copy):
        copy.start()
        started.append(copy)

    shard_up = copies.make("su", shard, shard, here.y_up)
    shard_down = copies.make("sd", shard, shard, here.y_down)
    shard_far = copies.make("sf", shard, shard, here.y_far)

    def group(steps, part):
        return wall.at[(here.z + GROUPS + steps) % GROUPS, pl.ds(2 * part, 2), c]

    def rise(n, part):
        return copies.make(("rise", n, part), group(-n, part), group(-n, part), here.z_up)

    def sink(n, part):
        return copies.make(("sink", n, part), group(n, part), group(n, part), here.z_down)

    def share(steps, part):
        return copies.make(("share", steps, part), group(steps, part), group(steps, part), here.partner)

    def forth(h):
        return copies.make(("forth", h), kv.at[4, h], kv.at[1, h], here.next_chip)

    def again(h):
        return copies.make(("again", h), kv.at[1, h], kv.at[3, h], here.next_chip)

    def back(h):
        return copies.make(("back", h), kv.at[4, h], relay.at[MINUS.index(h)], here.relay_to)

    def over(h):
        return copies.make(("over", h), relay.at[MINUS.index(h)], kv.at[3, h], here.pass_to)

    def twin_near(h):
        return copies.make(("near", h), kv.at[1, h], kv.at[2 * (1 - c), h], here.partner)

    def twin_far(h):
        return copies.make(("far", h), kv.at[4 - c, h], kv.at[2 * c, h], here.partner)

    def w_rows(block, first, count):
        return pl.ds(pl.multiple_of(block * WIDTH + c * HALF + first, 64), count)

    def w_cols(block):
        return pl.ds(pl.multiple_of(block * WIDTH, WIDTH), WIDTH)

    c_half = pl.ds(pl.multiple_of(c * HALF, HALF), HALF)
    w_right = copies.make("wr", wo_hbm.at[c_half, w_cols(right_x)], woc.at[w_rows(x, 0, HALF)], here.right)
    w_left = copies.make("wl", wo_hbm.at[c_half, w_cols(left_x)], woc.at[w_rows(x, 0, HALF)], here.left)
    w_far = copies.make("wf", wo_hbm.at[c_half, w_cols(far_x)], woc.at[w_rows(x, 0, HALF)], here.across)

    def w_twin(name, block):
        rows = w_rows(block, 0, HALF)
        return copies.make(("wt", name), woc.at[rows], woc.at[rows], here.partner)

    w_twin_l = w_twin("l", left_x)
    w_twin_r = w_twin("r", right_x)
    w_twin_f = w_twin("f", far_x)

    def ctx_cols(block, h):
        return pl.ds(pl.multiple_of(block * WIDTH + h * HEAD_DIM, HEAD_DIM), HEAD_DIM)

    def ctx_right(h):
        return copies.make(("cr", h), ctx.at[:, ctx_cols(x, h)], ctx.at[:, ctx_cols(x, h)], here.right)

    def ctx_left(h):
        return copies.make(("cl", h), ctx.at[:, ctx_cols(x, h)], ctx.at[:, ctx_cols(x, h)], here.left)

    def ctx_across(h):
        return copies.make(("ca", h), ctx.at[:, ctx_cols(x, h)], ctx.at[:, ctx_cols(x, h)], here.across)

    limits = key_limits(doc_ref, tail_ref, i)

    near_limit = jnp.where(c == 0, limits[1], limits[3])
    far_limit = jnp.where(c == 0, limits[3], limits[1])

    def own_keys(h):
        q = q_ref[:, h * HEAD_DIM:(h + 1) * HEAD_DIM]
        put_state(refs, h, flash_step(q, kv[4, h, 0], kv[4, h, 1], limits[0], None, "own"))

    def first_keys(h):
        q = q_ref[:, h * HEAD_DIM:(h + 1) * HEAD_DIM]
        state = flash_step(q, kv[1, h, 0], kv[1, h, 1], limits[2], get_state(refs, h))
        near = 2 * c
        state = flash_step(q, kv[near, h, 0], kv[near, h, 1], near_limit, state)
        put_state(refs, h, state)

    def last_keys(h):
        q = q_ref[:, h * HEAD_DIM:(h + 1) * HEAD_DIM]
        state = get_state(refs, h)
        state = flash_step(q, kv[3, h, 0], kv[3, h, 1], limits[4], state, "edge")
        far = 2 * (1 - c)
        state = flash_step(q, kv[far, h, 0], kv[far, h, 1], far_limit, state)
        ctx[:, ctx_cols(x, h)] = (state[2] / state[1]).astype(BF16)
        go(ctx_right(h))
        go(ctx_left(h))
        go(ctx_across(h))

    def take_context(h):
        ctx_right(h).wait_recv()
        ctx_left(h).wait_recv()
        ctx_across(h).wait_recv()

    def sunk(n, part, last=False):
        sink(n, part).wait_recv()
        if not last:
            go(sink(n + 1, part))
        go(share(n + 1, part))

    def risen(n, part, last=False):
        rise(n, part).wait_recv()
        if not last:
            go(rise(n + 1, part))
        go(share(-n - 1, part))

    for copy in shard_loads:
        copy.wait()
    shards = (shard_up, shard_down, shard_far)
    for copy in shards:
        copy.start()
    go(w_right)
    go(w_left)
    go(w_far)
    for copy in local[0] + local[1]:
        copy.wait()
    own_keys(0)
    own_keys(1)
    for h in (2, 3, 4, 5):
        for copy in local[h]:
            copy.wait()
    own_keys(2)
    for copy in shards:
        copy.wait_send()
    pl.semaphore_signal(clear_sem, inc=1, device_id=here.z_down, device_id_type=MESH)
    pl.semaphore_wait(clear_sem, 1)
    go(forth(0))
    go(back(1))
    go(forth(1))
    go(back(2))
    own_w.wait()
    for copy in shards:
        copy.wait_recv()
    for part in (0, 1):
        go(sink(0, part))
        go(share(0, part))
    for h in (3, 4, 5):
        own_keys(h)
    back(1).wait_recv()
    go(over(1))
    go(back(4))
    forth(0).wait_recv()
    go(again(0))
    go(forth(3))
    go(twin_near(0))
    twin_near(0).wait_recv()
    sunk(0, 0)
    first_keys(0)
    forth(1).wait_recv()
    go(forth(2))
    go(twin_near(1))
    sunk(0, 1)
    twin_near(1).wait_recv()
    first_keys(1)
    over(1).wait_recv()
    go(twin_far(1))
    again(0).wait_recv()
    go(twin_far(0))
    back(2).wait_recv()
    go(over(2))
    go(back(5))
    twin_far(1).wait_recv()
    last_keys(1)
    sunk(1, 0)
    twin_far(0).wait_recv()
    last_keys(0)
    w_right.wait_recv()
    go(w_twin_l)
    w_left.wait_recv()
    go(w_twin_r)
    w_far.wait_recv()
    go(w_twin_f)
    forth(3).wait_recv()
    go(again(3))
    go(forth(4))
    go(forth(5))
    go(twin_near(3))
    sunk(1, 1)
    twin_near(3).wait_recv()
    first_keys(3)
    forth(2).wait_recv()
    go(twin_near(2))
    back(4).wait_recv()
    go(over(4))
    sunk(2, 0)
    twin_near(2).wait_recv()
    first_keys(2)
    over(2).wait_recv()
    go(twin_far(2))
    twin_far(2).wait_recv()
    last_keys(2)
    back(5).wait_recv()
    go(over(5))
    again(3).wait_recv()
    go(twin_far(3))
    for part in (0, 1):
        go(rise(0, part))
    sunk(2, 1)
    twin_far(3).wait_recv()
    last_keys(3)
    forth(4).wait_recv()
    go(twin_near(4))
    twin_near(4).wait_recv()
    first_keys(4)
    over(4).wait_recv()
    go(twin_far(4))
    sunk(3, 0)
    twin_far(4).wait_recv()
    last_keys(4)
    forth(5).wait_recv()
    go(twin_near(5))
    twin_near(5).wait_recv()
    first_keys(5)
    over(5).wait_recv()
    go(twin_far(5))
    twin_far(5).wait_recv()
    last_keys(5)
    sunk(3, 1)
    for copy in (w_twin_l, w_twin_r, w_twin_f):
        copy.wait_recv()
    for h in range(4):
        take_context(h)

    def project(first, count, seed, store):
        def tile(t, carry):
            rows = pl.ds(pl.multiple_of(t * TILE, TILE), TILE)
            total = seed(rows)
            for block in range(4):
                at = block * WIDTH + first
                total = total + jnp.dot(
                    ctx[rows, at:at + count], woc[at:at + count, :], preferred_element_type=F32
                )
            store(rows, total)
            return carry

        lax.fori_loop(0, ROWS // TILE, tile, 0)

    def keep(rows, total):
        acc[rows, :] = total

    def cols(block):
        return pl.ds(pl.multiple_of(block * WIDTH, WIDTH), WIDTH)

    def finish(rows, total):
        tile = (res_ref[rows, :].astype(F32) + total).astype(BF16)
        hidden_ref[rows, :] = tile
        hid[rows, cols(x)] = tile

    project(0, 4 * HEAD_DIM, lambda rows: jnp.zeros((TILE, WIDTH), F32), keep)
    take_context(4)
    take_context(5)
    project(4 * HEAD_DIM, 2 * HEAD_DIM, lambda rows: acc[rows, :], finish)

    def part_rows(r):
        return pl.ds(r * TILE, TILE)

    def to_right(r):
        part = hid.at[part_rows(r), cols(x)]
        return copies.make(("r", r), part, part, here.right)

    def to_left(r):
        part = hid.at[part_rows(r), cols(x)]
        return copies.make(("l", r), part, part, here.left)

    def on_right(r):
        part = hid.at[pl.ds(r * TILE, TILE // 2), cols(left_x)]
        return copies.make(("or", r), part, part, here.right)

    def on_left(r):
        part = hid.at[pl.ds(r * TILE + TILE // 2, TILE // 2), cols(right_x)]
        return copies.make(("ol", r), part, part, here.left)

    def c_forth(r):
        return copies.make(("c_forth", r), cache.at[4, part_rows(r)], cache.at[1, part_rows(r)], here.next_chip)

    def c_again(r):
        return copies.make(("c_again", r), cache.at[1, part_rows(r)], cache.at[3, part_rows(r)], here.next_chip)

    def c_back(r):
        return copies.make(("c_back", r), cache.at[4, part_rows(r)], crelay.at[CACHE_MINUS.index(r)], here.relay_to)

    def c_over(r):
        return copies.make(("c_over", r), crelay.at[CACHE_MINUS.index(r)], cache.at[3, part_rows(r)], here.pass_to)

    def c_near(r):
        return copies.make(("c_near", r), cache.at[1, part_rows(r)], cache.at[2 * (1 - c), part_rows(r)], here.partner)

    def c_far(r):
        return copies.make(("c_far", r), cache.at[4 - c, part_rows(r)], cache.at[2 * c, part_rows(r)], here.partner)

    def hand_on(r):
        to_right(r).wait_recv()
        go(on_right(r))
        to_left(r).wait_recv()
        go(on_left(r))

    def send_part(r):
        go(to_right(r))
        go(to_left(r))

    def make_part(r):
        on_right(r).wait_recv()
        on_left(r).wait_recv()
        wide = hid[r * TILE:(r + 1) * TILE, :].astype(F32)
        mean_square = jnp.sum(wide * wide, axis=1, keepdims=True) / D
        normed = (wide * lax.rsqrt(mean_square + EPSILON) * gain_ref[...]).astype(BF16)
        made = jnp.dot(normed, wall[:, :, :, :, WIDTH:].reshape(D, CACHE), preferred_element_type=F32).astype(BF16)
        cache[4, r * TILE:(r + 1) * TILE, :] = made
        asked = jnp.dot(normed, wall[:, :, :, :, :WIDTH].reshape(D, WIDTH), preferred_element_type=F32).astype(BF16)
        queries[r * TILE:(r + 1) * TILE, :] = asked
        go(c_forth(r))
        if r in CACHE_MINUS:
            go(c_back(r))

    def c_arrive(r):
        c_forth(r).wait_recv()
        go(c_near(r))
        if r in CACHE_PLUS:
            go(c_again(r))
        else:
            c_back(r).wait_recv()
            go(c_over(r))

    def complete(r):
        (c_again if r in CACHE_PLUS else c_over)(r).wait_recv()
        go(c_far(r))

    send_part(0)
    send_part(1)
    risen(0, 0)
    risen(0, 1)
    sunk(4, 0, last=True)
    hand_on(0)
    send_part(2)
    sunk(4, 1, last=True)
    hand_on(1)
    send_part(3)
    risen(1, 0, last=True)
    risen(1, 1, last=True)
    for steps in range(-2, 6):
        for part in (0, 1):
            share(steps, part).wait_recv()
    make_part(0)
    hand_on(2)
    make_part(1)
    c_arrive(0)
    hand_on(3)
    make_part(2)
    c_arrive(1)
    complete(0)
    make_part(3)
    c_arrive(2)

    def head_cols(h):
        return pl.ds(pl.multiple_of(h * HEAD_DIM, HEAD_DIM), HEAD_DIM)

    def step(h, slot, limit, state, past=None):
        g = h // 3
        return flash_step(
            queries[:, head_cols(h)],
            cache[slot, :, head_cols(g)],
            cache[slot, :, head_cols(g + 2)],
            limit, state, past,
        )

    def c_own_keys(h, carry):
        put_state(refs, h, step(h, 4, limits[0], None, "own"))
        return carry

    lax.fori_loop(0, HEADS, c_own_keys, 0)
    c_arrive(3)
    complete(1)
    complete(2)
    for r in range(PARTS):
        c_near(r).wait_recv()

    def near_keys(h, carry):
        state = step(h, 1, limits[2], get_state(refs, h))
        put_state(refs, h, step(h, 2 * c, near_limit, state))
        return carry

    lax.fori_loop(0, HEADS, near_keys, 0)
    complete(3)
    for r in range(PARTS):
        c_far(r).wait_recv()

    def far_keys(h, carry):
        state = step(h, 3, limits[4], get_state(refs, h))
        state = step(h, 2 * (1 - c), far_limit, state)
        out_ref[:, head_cols(h)] = (state[2] / state[1]).astype(BF16)
        return carry

    lax.fori_loop(0, HEADS, far_keys, 0)
    for copy in started:
        copy.wait_send()
    assert len(copies.made) == N_COPIES, len(copies.made)


N_COPIES = 28 + 6 + 18 + 3 + 10 + 4 + 16 + 16 + 18


def layer(doc, tail, q, res, gain, k, v, wo, wq, wc):
    any_spec = pl.BlockSpec(memory_space=pl.ANY)
    vmem = pl.BlockSpec(memory_space=pltpu.VMEM)
    smem = pl.BlockSpec(memory_space=pltpu.SMEM)
    return pl.pallas_call(
        layer_kernel,
        out_shape=(jax.ShapeDtypeStruct((ROWS, WIDTH), BF16),) * 2,
        in_specs=[smem, smem, vmem, vmem, vmem] + [any_spec] * 5,
        out_specs=(vmem, vmem),
        scratch_shapes=[
            pltpu.VMEM((SLOTS, HEADS, 2, ROWS, HEAD_DIM), BF16),
            pltpu.VMEM((len(MINUS), 2, ROWS, HEAD_DIM), BF16),
            pltpu.VMEM((ROWS, D), BF16),
            pltpu.VMEM((D, WIDTH), BF16),
            pltpu.VMEM((ROWS, WIDTH), F32),
            *STATE,
            pltpu.VMEM((ROWS, D), BF16),
            pltpu.VMEM((GROUPS, 4, 2, SHARD, COLS), BF16),
            pltpu.VMEM((SLOTS, ROWS, CACHE), BF16),
            pltpu.VMEM((len(CACHE_MINUS), TILE, CACHE), BF16),
            pltpu.VMEM((ROWS, WIDTH), BF16),
            pltpu.SemaphoreType.DMA((2 * HEADS + 3,)),
            pltpu.SemaphoreType.DMA((N_COPIES,)),
            pltpu.SemaphoreType.DMA((N_COPIES,)),
            pltpu.SemaphoreType.REGULAR,
        ],
        compiler_params=pltpu.CompilerParams(
            collective_id=0, has_side_effects=True, vmem_limit_bytes=60 * 1024 * 1024
        ),
        name="layer",
    )(doc, tail, q, res, gain, k, v, wo, wq, wc)


def local(
    residual, q_self, k_self, v_self, w_out, norm_gain, w_query, w_cache, block_doc, tail_len
):
    return layer(
        block_doc, tail_len, q_self, residual, norm_gain.reshape(1, D),
        k_self, v_self, w_out, w_query, w_cache,
    )


def solution(mesh):
    in_specs = (
        P("seq", "head"),
        P("seq", "head"),
        P("seq", "head"),
        P("seq", "head"),
        P("head", None),
        P(),
        P("seq", "head"),
        P("seq", "head"),
        P(),
        P(),
    )
    out_specs = (P("seq", "head"), P("seq", "head"))
    return jax.shard_map(local, mesh=mesh, in_specs=in_specs, out_specs=out_specs, check_vma=False)
```

```python
import functools
import math

import jax
import jax.numpy as jnp
from jax import lax
from jax.experimental import pallas as pl
from jax.experimental.pallas import tpu as pltpu
from jax.sharding import PartitionSpec as P

D = 3072
HEAD_DIM = 128
ROWS = 512
NBLK = 64
HEADS = 6
SLOTS = 5
WIDTH = HEADS * HEAD_DIM
HALF = WIDTH // 2
EPSILON = 1e-06
SCALE = 1.0 / math.sqrt(HEAD_DIM)
EXP2_SCALE = SCALE * math.log2(math.e)
MASKED = -1e30
LARGE = 3.0e38
TILE = 128
GROUPS = 8
SHARD = D // NBLK
COLS = WIDTH + 2 * 2 * HEAD_DIM

MESH = pl.DeviceIdType.MESH
F32 = jnp.float32
BF16 = jnp.bfloat16

PLUS = (0, 3)
MINUS = (1, 2, 4, 5)


PARTS = ROWS // TILE
CACHE = 2 * 2 * HEAD_DIM
CACHE_PLUS = (0, 2)
CACHE_MINUS = (1, 3)


class Copies:
    def __init__(self, send_sem, recv_sem):
        self.send_sem, self.recv_sem = send_sem, recv_sem
        self.made = {}

    def make(self, name, src, dst, device):
        if name not in self.made:
            self.made[name] = len(self.made)
        n = self.made[name]
        return pltpu.make_async_remote_copy(
            src_ref=src,
            dst_ref=dst,
            send_sem=self.send_sem.at[n],
            recv_sem=self.recv_sem.at[n],
            device_id=device,
            device_id_type=MESH,
        )


class Place:
    def __init__(self):
        i = lax.axis_index("seq")
        x = lax.axis_index("head")
        self.i, self.x = i, x
        c = i % 2
        y = (i // 2) % 4
        z = i // 8
        self.c, self.y, self.z = c, y, z

        def at(zz, yy, cc):
            return ((zz + 8) % 8 * 4 + yy) * 2 + cc

        up = (y + 1) % 4
        down = (y + 3) % 4
        self.next_chip = (at(z + (y + 1) // 4, up, c), x)
        self.prev_chip = (at(z - (6 - y) // 6, down, c), x)
        self.relay_to = (at(z, down, c), x)
        self.relay_from = (at(z, up, c), x)
        self.pass_to = (at(z + (up + 2) // 4, down, c), x)
        self.pass_from = (at(z - ((y + 2) % 4) // 2, up, c), x)
        self.partner = (i + 1 - 2 * c, x)
        self.right = (i, (x + 1) % 4)
        self.left = (i, (x + 3) % 4)
        self.across = (i, (x + 2) % 4)
        self.y_up, self.y_down = (at(z, up, c), x), (at(z, down, c), x)
        self.y_far = (at(z, (y + 2) % 4, c), x)
        self.z_up, self.z_down = (at(z + 1, y, c), x), (at(z - 1, y, c), x)


def greet(devices):
    barrier = pltpu.get_barrier_semaphore()
    for device in devices:
        pl.semaphore_signal(barrier, inc=1, device_id=device, device_id_type=MESH)
    pl.semaphore_wait(barrier, len(devices))


def key_limits(doc_ref, tail_ref, i):
    limits = []
    own = doc_ref[i]
    for d in range(SLOTS):
        j = jnp.maximum(i - d, 0)
        doc = doc_ref[j]
        after = doc_ref[jnp.minimum(j + 1, NBLK - 1)]
        closing = jnp.logical_or(j == NBLK - 1, after != doc)
        count = jnp.where(closing, tail_ref[j], ROWS)
        seen = jnp.logical_and(i - d >= 0, doc == own)
        limits.append(jnp.where(seen, count, 0))
    return limits


def flash_step(q, keys, values, limit, state, past=None, first=0):
    rows, count = q.shape[0], keys.shape[0]
    lane = lax.broadcasted_iota(jnp.int32, (1, count), 1)
    s = lax.dot_general(q, keys, (((1,), (1,)), ((), ())), preferred_element_type=F32)
    s = jnp.minimum(s, jnp.where(lane < limit, LARGE, MASKED))
    if past is not None:
        query_at = first + lax.broadcasted_iota(jnp.int32, (rows, count), 0)
        key_at = lax.broadcasted_iota(jnp.int32, (rows, count), 1)
        s = jnp.where(key_at <= query_at if past == "own" else key_at > query_at, s, MASKED)
    peak = jnp.max(s, axis=1, keepdims=True)
    if state is not None:
        peak = jnp.maximum(peak, state[0])
    spread = peak if peak.shape[1] == 1 else jnp.concatenate([peak] * (count // HEAD_DIM), axis=1)
    weights = jnp.exp2((s - spread) * EXP2_SCALE)
    total = jnp.sum(weights, axis=1, keepdims=True)
    blended = jnp.dot(weights.astype(BF16), values, preferred_element_type=F32)
    if state is not None:
        shrink = jnp.exp2((state[0] - peak) * EXP2_SCALE)
        total = state[1] * shrink + total
        blended = state[2] * shrink + blended
    return peak, total, blended


def put_state(refs, h, state, rows=slice(0, ROWS)):
    peak_ref, total_ref, blended_ref = refs
    peak_ref[h, rows] = jnp.broadcast_to(state[0], state[2].shape)
    total_ref[h, rows] = jnp.broadcast_to(state[1], state[2].shape)
    blended_ref[h, rows] = state[2]


def get_state(refs, h):
    peak_ref, total_ref, blended_ref = refs
    return peak_ref[h], total_ref[h], blended_ref[h]


STATE = [
    pltpu.VMEM((HEADS, ROWS, HEAD_DIM), F32),
    pltpu.VMEM((HEADS, ROWS, HEAD_DIM), F32),
    pltpu.VMEM((HEADS, ROWS, HEAD_DIM), F32),
]


def layer_kernel(
    doc_ref, tail_ref, gain_ref, q_hbm, res_hbm, k_hbm, v_hbm, wo_hbm, wq_hbm, wc_hbm,
    hidden_hbm, out_hbm, q_ref, res_ref, out_ref,
    kv, relay, ctx, woc, acc, peak_ref, total_ref, blended_ref,
    hid, wall, cache, crelay, queries, local_sem, send_sem, recv_sem, clear_sem,
):
    refs = (peak_ref, total_ref, blended_ref)
    here = Place()
    i, x, c = here.i, here.x, here.c
    copies = Copies(send_sem, recv_sem)
    started = []
    right_x, left_x, far_x = (x + 1) % 4, (x + 3) % 4, (x + 2) % 4

    load_q = pltpu.make_async_copy(q_hbm, q_ref, local_sem.at[2 * HEADS + 3])
    load_q.start()
    local = []
    for h in range(HEADS):
        cols = pl.ds(h * HEAD_DIM, HEAD_DIM)
        one = pltpu.make_async_copy(k_hbm.at[:, cols], kv.at[SLOTS - 1, h, 0], local_sem.at[2 * h])
        two = pltpu.make_async_copy(v_hbm.at[:, cols], kv.at[SLOTS - 1, h, 1], local_sem.at[2 * h + 1])
        one.start()
        two.start()
        local.append((one, two))
    own_rows = pl.ds(pl.multiple_of(x * WIDTH, WIDTH), WIDTH)
    own_cols = pl.ds(pl.multiple_of(x * WIDTH, WIDTH), WIDTH)
    own_w = pltpu.make_async_copy(wo_hbm.at[:, own_cols], woc.at[own_rows], local_sem.at[2 * HEADS])
    own_w.start()
    shard = wall.at[here.z, here.y, c]
    shard_loads = (
        pltpu.make_async_copy(wq_hbm, shard.at[:, pl.ds(0, WIDTH)], local_sem.at[2 * HEADS + 1]),
        pltpu.make_async_copy(wc_hbm, shard.at[:, pl.ds(WIDTH, CACHE)], local_sem.at[2 * HEADS + 2]),
    )
    for copy in shard_loads:
        copy.start()
    load_res = pltpu.make_async_copy(res_hbm, res_ref, local_sem.at[2 * HEADS + 4])
    load_res.start()

    greet([
        here.next_chip, here.prev_chip, here.relay_to, here.relay_from, here.pass_to, here.pass_from,
        here.partner, here.right, here.left, here.across, here.across, here.y_up, here.y_down, here.y_far, here.y_far, here.z_up, here.z_down,
    ])

    def go(copy):
        copy.start()
        started.append(copy)

    shard_up = copies.make("su", shard, shard, here.y_up)
    shard_down = copies.make("sd", shard, shard, here.y_down)
    shard_far = copies.make("sf", shard, shard, here.y_far)

    def group(steps, part):
        return wall.at[(here.z + GROUPS + steps) % GROUPS, pl.ds(2 * part, 2), c]

    def rise(n, part):
        return copies.make(("rise", n, part), group(-n, part), group(-n, part), here.z_up)

    def sink(n, part):
        return copies.make(("sink", n, part), group(n, part), group(n, part), here.z_down)

    def share(steps, part):
        return copies.make(("share", steps, part), group(steps, part), group(steps, part), here.partner)

    def forth(h):
        return copies.make(("forth", h), kv.at[4, h], kv.at[1, h], here.next_chip)

    def again(h):
        return copies.make(("again", h), kv.at[1, h], kv.at[3, h], here.next_chip)

    def back(h):
        return copies.make(("back", h), kv.at[4, h], relay.at[MINUS.index(h)], here.relay_to)

    def over(h):
        return copies.make(("over", h), relay.at[MINUS.index(h)], kv.at[3, h], here.pass_to)

    def twin_near(h):
        return copies.make(("near", h), kv.at[1, h], kv.at[2 * (1 - c), h], here.partner)

    def twin_far(h):
        return copies.make(("far", h), kv.at[4 - c, h], kv.at[2 * c, h], here.partner)

    def w_rows(block, first, count):
        return pl.ds(pl.multiple_of(block * WIDTH + c * HALF + first, 64), count)

    def w_cols(block):
        return pl.ds(pl.multiple_of(block * WIDTH, WIDTH), WIDTH)

    c_half = pl.ds(pl.multiple_of(c * HALF, HALF), HALF)
    w_right = copies.make("wr", wo_hbm.at[c_half, w_cols(right_x)], woc.at[w_rows(x, 0, HALF)], here.right)
    w_left = copies.make("wl", wo_hbm.at[c_half, w_cols(left_x)], woc.at[w_rows(x, 0, HALF)], here.left)
    w_far = copies.make("wf", wo_hbm.at[c_half, w_cols(far_x)], woc.at[w_rows(x, 0, HALF)], here.across)

    def w_twin(name, block):
        rows = w_rows(block, 0, HALF)
        return copies.make(("wt", name), woc.at[rows], woc.at[rows], here.partner)

    w_twin_l = w_twin("l", left_x)
    w_twin_r = w_twin("r", right_x)
    w_twin_f = w_twin("f", far_x)

    def ctx_cols(block, h):
        return pl.ds(pl.multiple_of(block * WIDTH + h * HEAD_DIM, HEAD_DIM), HEAD_DIM)

    def ctx_right(h):
        return copies.make(("cr", h), ctx.at[:, ctx_cols(x, h)], ctx.at[:, ctx_cols(x, h)], here.right)

    def ctx_left(h):
        return copies.make(("cl", h), ctx.at[:, ctx_cols(x, h)], ctx.at[:, ctx_cols(x, h)], here.left)

    def ctx_across(h):
        return copies.make(("ca", h), ctx.at[:, ctx_cols(x, h)], ctx.at[:, ctx_cols(x, h)], here.across)

    limits = key_limits(doc_ref, tail_ref, i)

    near_limit = jnp.where(c == 0, limits[1], limits[3])
    far_limit = jnp.where(c == 0, limits[3], limits[1])

    def own_keys(h):
        q = q_ref[:, h * HEAD_DIM:(h + 1) * HEAD_DIM]
        put_state(refs, h, flash_step(q, kv[4, h, 0], kv[4, h, 1], limits[0], None, "own"))

    def first_keys(h):
        q = q_ref[:, h * HEAD_DIM:(h + 1) * HEAD_DIM]
        state = flash_step(q, kv[1, h, 0], kv[1, h, 1], limits[2], get_state(refs, h))
        near = 2 * c
        state = flash_step(q, kv[near, h, 0], kv[near, h, 1], near_limit, state)
        put_state(refs, h, state)

    def last_keys(h):
        q = q_ref[:, h * HEAD_DIM:(h + 1) * HEAD_DIM]
        state = get_state(refs, h)
        state = flash_step(q, kv[3, h, 0], kv[3, h, 1], limits[4], state, "edge")
        far = 2 * (1 - c)
        state = flash_step(q, kv[far, h, 0], kv[far, h, 1], far_limit, state)
        ctx[:, ctx_cols(x, h)] = (state[2] / state[1]).astype(BF16)
        go(ctx_right(h))
        go(ctx_left(h))
        go(ctx_across(h))

    def take_context(h):
        ctx_right(h).wait_recv()
        ctx_left(h).wait_recv()
        ctx_across(h).wait_recv()

    def sunk(n, part, last=False):
        sink(n, part).wait_recv()
        if not last:
            go(sink(n + 1, part))
        go(share(n + 1, part))

    def risen(n, part, last=False):
        rise(n, part).wait_recv()
        if not last:
            go(rise(n + 1, part))
        go(share(-n - 1, part))

    for copy in shard_loads:
        copy.wait()
    shards = (shard_up, shard_down, shard_far)
    for copy in shards:
        copy.start()
    go(w_right)
    go(w_left)
    go(w_far)
    for copy in local[0] + local[1]:
        copy.wait()
    load_q.wait()
    own_keys(0)
    own_keys(1)
    for h in (2, 3, 4, 5):
        for copy in local[h]:
            copy.wait()
    own_keys(2)
    for copy in shards:
        copy.wait_send()
    pl.semaphore_signal(clear_sem, inc=1, device_id=here.z_down, device_id_type=MESH)
    pl.semaphore_wait(clear_sem, 1)
    go(forth(0))
    go(back(1))
    go(forth(1))
    go(back(2))
    own_w.wait()
    for copy in shards:
        copy.wait_recv()
    for part in (0, 1):
        go(sink(0, part))
        go(share(0, part))
    for h in (3, 4, 5):
        own_keys(h)
    back(1).wait_recv()
    go(over(1))
    go(back(4))
    forth(0).wait_recv()
    go(again(0))
    go(forth(3))
    go(twin_near(0))
    twin_near(0).wait_recv()
    sunk(0, 0)
    first_keys(0)
    forth(1).wait_recv()
    go(forth(2))
    go(twin_near(1))
    sunk(0, 1)
    twin_near(1).wait_recv()
    first_keys(1)
    over(1).wait_recv()
    go(twin_far(1))
    again(0).wait_recv()
    go(twin_far(0))
    back(2).wait_recv()
    go(over(2))
    go(back(5))
    twin_far(1).wait_recv()
    last_keys(1)
    sunk(1, 0)
    twin_far(0).wait_recv()
    last_keys(0)
    w_right.wait_recv()
    go(w_twin_l)
    w_left.wait_recv()
    go(w_twin_r)
    w_far.wait_recv()
    go(w_twin_f)
    forth(3).wait_recv()
    go(again(3))
    go(forth(4))
    go(forth(5))
    go(twin_near(3))
    sunk(1, 1)
    twin_near(3).wait_recv()
    first_keys(3)
    forth(2).wait_recv()
    go(twin_near(2))
    back(4).wait_recv()
    go(over(4))
    sunk(2, 0)
    twin_near(2).wait_recv()
    first_keys(2)
    over(2).wait_recv()
    go(twin_far(2))
    twin_far(2).wait_recv()
    last_keys(2)
    back(5).wait_recv()
    go(over(5))
    again(3).wait_recv()
    go(twin_far(3))
    for part in (0, 1):
        go(rise(0, part))
    sunk(2, 1)
    twin_far(3).wait_recv()
    last_keys(3)
    forth(4).wait_recv()
    go(twin_near(4))
    twin_near(4).wait_recv()
    first_keys(4)
    over(4).wait_recv()
    go(twin_far(4))
    sunk(3, 0)
    twin_far(4).wait_recv()
    last_keys(4)
    forth(5).wait_recv()
    go(twin_near(5))
    twin_near(5).wait_recv()
    first_keys(5)
    over(5).wait_recv()
    go(twin_far(5))
    twin_far(5).wait_recv()
    last_keys(5)
    sunk(3, 1)
    for copy in (w_twin_l, w_twin_r, w_twin_f):
        copy.wait_recv()
    for h in range(4):
        take_context(h)

    def project_tile(t, first, count, seed, store):
        rows = pl.ds(pl.multiple_of(t * TILE, TILE), TILE)
        total = seed(rows)
        for block in range(4):
            at = block * WIDTH + first
            total = total + jnp.dot(
                ctx[rows, at:at + count], woc[at:at + count, :], preferred_element_type=F32
            )
        store(rows, total)

    def keep(rows, total):
        acc[rows, :] = total

    def cols(block):
        return pl.ds(pl.multiple_of(block * WIDTH, WIDTH), WIDTH)

    def finish(rows, total):
        tile = (res_ref[rows, :].astype(F32) + total).astype(BF16)
        hid[rows, cols(x)] = tile

    def early(t, carry):
        project_tile(t, 0, 4 * HEAD_DIM, lambda rows: jnp.zeros((TILE, WIDTH), F32), keep)
        return carry

    def late(t):
        project_tile(t, 4 * HEAD_DIM, 2 * HEAD_DIM, lambda rows: acc[rows, :], finish)

    lax.fori_loop(0, PARTS, early, 0)
    take_context(4)
    risen(0, 0)
    take_context(5)

    def part_rows(r):
        return pl.ds(r * TILE, TILE)

    def to_right(r):
        part = hid.at[part_rows(r), cols(x)]
        return copies.make(("r", r), part, part, here.right)

    def to_left(r):
        part = hid.at[part_rows(r), cols(x)]
        return copies.make(("l", r), part, part, here.left)

    def on_right(r):
        part = hid.at[pl.ds(r * TILE, TILE // 2), cols(left_x)]
        return copies.make(("or", r), part, part, here.right)

    def on_left(r):
        part = hid.at[pl.ds(r * TILE + TILE // 2, TILE // 2), cols(right_x)]
        return copies.make(("ol", r), part, part, here.left)

    def c_forth(r):
        return copies.make(("c_forth", r), cache.at[4, part_rows(r)], cache.at[1, part_rows(r)], here.next_chip)

    def c_again(r):
        return copies.make(("c_again", r), cache.at[1, part_rows(r)], cache.at[3, part_rows(r)], here.next_chip)

    def c_back(r):
        return copies.make(("c_back", r), cache.at[4, part_rows(r)], crelay.at[CACHE_MINUS.index(r)], here.relay_to)

    def c_over(r):
        return copies.make(("c_over", r), crelay.at[CACHE_MINUS.index(r)], cache.at[3, part_rows(r)], here.pass_to)

    def c_near(r):
        return copies.make(("c_near", r), cache.at[1, part_rows(r)], cache.at[2 * (1 - c), part_rows(r)], here.partner)

    def c_far(r):
        return copies.make(("c_far", r), cache.at[4 - c, part_rows(r)], cache.at[2 * c, part_rows(r)], here.partner)

    def hand_on(r):
        to_right(r).wait_recv()
        go(on_right(r))
        to_left(r).wait_recv()
        go(on_left(r))

    def send_part(r):
        go(to_right(r))
        go(to_left(r))

    def make_part(r):
        on_right(r).wait_recv()
        on_left(r).wait_recv()
        wide = hid[r * TILE:(r + 1) * TILE, :].astype(F32)
        mean_square = jnp.sum(wide * wide, axis=1, keepdims=True) / D
        normed = (wide * lax.rsqrt(mean_square + EPSILON) * gain_ref[...]).astype(BF16)
        made = jnp.dot(normed, wall[:, :, :, :, WIDTH:].reshape(D, CACHE), preferred_element_type=F32).astype(BF16)
        cache[4, r * TILE:(r + 1) * TILE, :] = made
        asked = jnp.dot(normed, wall[:, :, :, :, :WIDTH].reshape(D, WIDTH), preferred_element_type=F32).astype(BF16)
        queries[r * TILE:(r + 1) * TILE, :] = asked
        go(c_forth(r))
        if r in CACHE_MINUS:
            go(c_back(r))

    def c_arrive(r):
        c_forth(r).wait_recv()
        go(c_near(r))
        if r in CACHE_PLUS:
            go(c_again(r))
        else:
            c_back(r).wait_recv()
            go(c_over(r))

    def complete(r):
        (c_again if r in CACHE_PLUS else c_over)(r).wait_recv()
        go(c_far(r))

    load_res.wait()
    late(0)
    send_part(0)
    late(1)
    send_part(1)
    late(2)
    late(3)
    save_hidden = pltpu.make_async_copy(hid.at[:, cols(x)], hidden_hbm, local_sem.at[2 * HEADS + 5])
    save_hidden.start()
    risen(0, 1)
    sunk(4, 0, last=True)
    hand_on(0)
    send_part(2)
    sunk(4, 1, last=True)
    hand_on(1)
    send_part(3)
    risen(1, 0, last=True)
    risen(1, 1, last=True)
    for steps in range(-2, 6):
        for part in (0, 1):
            share(steps, part).wait_recv()
    def head_cols(h):
        return pl.ds(pl.multiple_of(h * HEAD_DIM, HEAD_DIM), HEAD_DIM)

    half = ROWS // 2

    def c_own_first(h, carry):
        g = h // 3
        state = flash_step(
            queries[:half, head_cols(h)],
            cache[4, :half, head_cols(g)],
            cache[4, :half, head_cols(g + 2)],
            limits[0], None, "own",
        )
        put_state(refs, h, state, slice(0, half))
        return carry

    def c_own_last(h, carry):
        g = h // 3
        state = flash_step(
            queries[half:, head_cols(h)],
            cache[4, :, head_cols(g)],
            cache[4, :, head_cols(g + 2)],
            limits[0], None, "own", half,
        )
        put_state(refs, h, state, slice(half, ROWS))
        return carry

    def step(h, slot, limit, state, past=None):
        g = h // 3
        return flash_step(
            queries[:, head_cols(h)],
            cache[slot, :, head_cols(g)],
            cache[slot, :, head_cols(g + 2)],
            limit, state, past,
        )

    make_part(0)
    hand_on(2)
    make_part(1)
    c_arrive(0)
    lax.fori_loop(0, HEADS, c_own_first, 0)
    hand_on(3)
    make_part(2)
    c_arrive(1)
    complete(0)
    make_part(3)
    lax.fori_loop(0, HEADS, c_own_last, 0)
    c_arrive(2)
    c_forth(3).wait_recv()
    go(c_near(3))

    def line_keys(h, carry):
        put_state(refs, h, step(h, 1, limits[2], get_state(refs, h)))
        return carry

    lax.fori_loop(0, HEADS, line_keys, 0)
    c_back(3).wait_recv()
    go(c_over(3))
    complete(1)
    complete(2)
    for r in range(PARTS):
        c_near(r).wait_recv()

    def near_keys(h, carry):
        put_state(refs, h, step(h, 2 * c, near_limit, get_state(refs, h)))
        return carry

    lax.fori_loop(0, HEADS, near_keys, 0)
    complete(3)
    for r in range(PARTS):
        c_far(r).wait_recv()

    def save(h):
        return pltpu.make_async_copy(
            out_ref.at[:, head_cols(h)], out_hbm.at[:, head_cols(h)], local_sem.at[2 * HEADS + 6 + h]
        )

    def far_keys(h, carry):
        state = step(h, 3, limits[4], get_state(refs, h))
        state = step(h, 2 * (1 - c), far_limit, state)
        out_ref[:, head_cols(h)] = (state[2] / state[1]).astype(BF16)
        save(h).start()
        return carry

    lax.fori_loop(0, HEADS, far_keys, 0)
    save_hidden.wait()
    for h in range(HEADS):
        save(h).wait()
    for copy in started:
        copy.wait_send()
    assert len(copies.made) == N_COPIES, len(copies.made)


N_COPIES = 28 + 6 + 18 + 3 + 10 + 4 + 16 + 16 + 18


def layer(doc, tail, gain, q, res, k, v, wo, wq, wc):
    any_spec = pl.BlockSpec(memory_space=pl.ANY)
    vmem = pl.BlockSpec(memory_space=pltpu.VMEM)
    smem = pl.BlockSpec(memory_space=pltpu.SMEM)
    return pl.pallas_call(
        layer_kernel,
        out_shape=(jax.ShapeDtypeStruct((ROWS, WIDTH), BF16),) * 2,
        in_specs=[smem, smem, vmem] + [any_spec] * 7,
        out_specs=(any_spec, any_spec),
        scratch_shapes=[
            pltpu.VMEM((ROWS, WIDTH), BF16),
            pltpu.VMEM((ROWS, WIDTH), BF16),
            pltpu.VMEM((ROWS, WIDTH), BF16),
            pltpu.VMEM((SLOTS, HEADS, 2, ROWS, HEAD_DIM), BF16),
            pltpu.VMEM((len(MINUS), 2, ROWS, HEAD_DIM), BF16),
            pltpu.VMEM((ROWS, D), BF16),
            pltpu.VMEM((D, WIDTH), BF16),
            pltpu.VMEM((ROWS, WIDTH), F32),
            *STATE,
            pltpu.VMEM((ROWS, D), BF16),
            pltpu.VMEM((GROUPS, 4, 2, SHARD, COLS), BF16),
            pltpu.VMEM((SLOTS, ROWS, CACHE), BF16),
            pltpu.VMEM((len(CACHE_MINUS), TILE, CACHE), BF16),
            pltpu.VMEM((ROWS, WIDTH), BF16),
            pltpu.SemaphoreType.DMA((3 * HEADS + 6,)),
            pltpu.SemaphoreType.DMA((N_COPIES,)),
            pltpu.SemaphoreType.DMA((N_COPIES,)),
            pltpu.SemaphoreType.REGULAR,
        ],
        compiler_params=pltpu.CompilerParams(
            collective_id=0, has_side_effects=True, vmem_limit_bytes=60 * 1024 * 1024
        ),
        name="layer",
    )(doc, tail, gain, q, res, k, v, wo, wq, wc)


def local(
    residual, q_self, k_self, v_self, w_out, norm_gain, w_query, w_cache, block_doc, tail_len
):
    return layer(
        block_doc, tail_len, norm_gain.reshape(1, D), q_self, residual, k_self, v_self,
        w_out, w_query, w_cache,
    )


def solution(mesh):
    in_specs = (
        P("seq", "head"),
        P("seq", "head"),
        P("seq", "head"),
        P("seq", "head"),
        P("head", None),
        P(),
        P("seq", "head"),
        P("seq", "head"),
        P(),
        P(),
    )
    out_specs = (P("seq", "head"), P("seq", "head"))
    return jax.shard_map(local, mesh=mesh, in_specs=in_specs, out_specs=out_specs, check_vma=False)
```
